32 devices in a mesh: spin: 2 (over x), row: 4 (over z), col: 4 (over y, core).
Axes of the slice: x: 2, y: 2, z: 4, core: 2. Of those that a mesh axis runs over, the one named last changes fastest.
Arguments:
- hamiltonian: float32 [5120, 2560], P(('spin', 'row'), 'col'), parts along dimension 0
- bounds: float32 [4], P('spin'), parts along dimension 0
- occ_count: int32 [2], P('spin'), parts along dimension 0
- branches: int32 [12], P('spin'), parts along dimension 0
Outputs:
- output 1: float32 [5120, 2560], P(('spin', 'row'), 'col'), parts along dimension 0
- output 2: float32 [12], P('spin'), parts along dimension 0
- output 3: float32 [2], P('spin'), parts along dimension 0
There are 2 independent parts. The reference program is written for one: setup_inputs(seed, part) draws one part's arguments, and reference() takes and returns one part's arrays. A program takes and returns all parts, laid end to end along the dimension named above; each array names one.
All inputs are finite; a program needn't handle non-finite values.
Results may differ from the reference program's by a relative error of at most 0.001.
Values sent between devices are 32-bit elements.
A program may use at most 1 GiB of HBM per device.

```python
import jax
import jax.numpy as jnp
from jax import lax

N = 2560
STEPS = 6


def setup_inputs(seed: int = 0, part: int = 0) -> dict:
    base_key = jax.random.fold_in(jax.random.key(seed), part)
    key_ham, key_slack, key_occ, key_bits, key_perm = jax.random.split(base_key, 5)
    gauss_mat = jax.random.normal(key_ham, (N, N), jnp.float32)
    center = -2.0
    hamiltonian = (gauss_mat + gauss_mat.T) * (0.5 / N) ** 0.5 + center * jnp.eye(N, dtype=jnp.float32)
    slack_vals = jax.random.uniform(key_slack, (2,), jnp.float32, 0.1, 0.6)
    bounds = jnp.stack([center - 2.0 * (1.0 + slack_vals[0]), center + 2.0 * (1.0 + slack_vals[1])])
    occ_count = jax.random.randint(key_occ, (1,), (3 * N) // 20, (3 * N) // 8 + 1, jnp.int32)
    extra_bits = jax.random.randint(key_bits, (STEPS - 4,), 0, 2, jnp.int32)
    flag_pool = jnp.concatenate([jnp.zeros((2,), jnp.int32), jnp.ones((2,), jnp.int32), extra_bits])
    branches = jax.random.permutation(key_perm, flag_pool)
    return {"hamiltonian": hamiltonian, "bounds": bounds, "occ_count": occ_count, "branches": branches}


def reference(hamiltonian, bounds, occ_count, branches):
    identity = jnp.eye(N, dtype=jnp.float32)
    chem_pot = jnp.trace(hamiltonian) / N
    occupied = occ_count[0].astype(jnp.float32)
    scale_fac = jnp.minimum(occupied / (bounds[1] - chem_pot), (N - occupied) / (chem_pot - bounds[0]))
    density = (scale_fac / N) * (chem_pot * identity - hamiltonian) + (occupied / N) * identity

    def sp2_step(current, branch_flag):
        occupation = jnp.sum(current * current)
        squared = jnp.dot(current, current, preferred_element_type=jnp.float32)
        updated = jnp.where(branch_flag == 1, squared, 2.0 * current - squared)
        return updated, occupation

    density, occupations = lax.scan(sp2_step, density, branches)
    energy = 2.0 * jnp.sum(density * hamiltonian)
    return density, occupations, energy.reshape(1)
```

```python
import functools

import jax
import jax.numpy as jnp
from jax import lax
from jax.experimental import pallas as pl
from jax.experimental.pallas import tpu as pltpu
from jax.sharding import PartitionSpec as P

F32 = jnp.float32
BF16 = jnp.bfloat16
MESH = pl.DeviceIdType.MESH
TERMS = ((0, 2), (2, 0), (1, 1), (0, 1), (1, 0), (0, 0))
NN = (((1,), (0,)), ((), ()))
NT = (((1,), (1,)), ((), ()))


def slab_of(label):
    return label // 2 + 2 * (1 - label % 2)


def kernel(steps, h_ref, bounds_ref, count_ref, flag_ref, out_ref, occ_ref, energy_ref,
           X, D, S, stats, part0, part1, g_send, g_recv, send, recv_x, recv_d, credit, p_send, p_recv):
    blk = h_ref.shape[0]
    T = 2 * blk // 5
    HB = 2 * blk
    order = 4 * blk
    sid, z, col = lax.axis_index("spin"), lax.axis_index("row"), lax.axis_index("col")
    y, c = col // 2, col % 2
    half = z // 2
    u = (y + half) % 2
    inner = (z + 1) // 2 % 2
    inner = jnp.int32(inner)
    sib_col, yp_col, sib_yp_col = 2 * y + 1 - c, 2 * (1 - y) + c, 2 * (1 - y) + 1 - c
    zp = z + 1 - 2 * (z % 2)
    opp = 3 - z
    outer = 3 * (z // 2)
    inner_z = 1 + half
    me = z * 4 + col

    def dev(zz, cc):
        return (sid, zz, cc)

    sib, ypart, zpart = dev(z, sib_col), dev(z, yp_col), dev(zp, col)

    def copy(src, dst, s_sem, r_sem, device):
        return pltpu.make_async_remote_copy(src_ref=src, dst_ref=dst, send_sem=s_sem, recv_sem=r_sem,
                                            device_id=device, device_id_type=MESH)

    def wait_recv(dst, r_sem):
        copy(dst, dst, g_send.at[0], r_sem, sib).wait_recv()

    def wait_send(src, s_sem):
        copy(src, src, s_sem, g_recv.at[0], sib).wait_send()

    def ds(index, size, step=None):
        return pl.ds(pl.multiple_of(index * (step or size), step or size), size)

    def block_at(zz, cc):
        row = (zz % 2) * blk
        column = ((cc // 2 + zz // 2) % 2) * HB + (cc % 2) * blk
        return X.at[0, pl.ds(pl.multiple_of(row, blk), blk), pl.ds(pl.multiple_of(column, blk), blk)]

    own_rows = ds(z % 2, blk)
    own_cols = ds(2 * u + c, blk)

    barrier = pltpu.get_barrier_semaphore()
    for dz in range(4):
        for dc in range(4):
            if dz or dc:
                pl.semaphore_signal(barrier, inc=1, device_id=dev((z + dz) % 4, (col + dc) % 4), device_id_type=MESH)
    pl.semaphore_wait(barrier, 15)

    def share(part):
        index = 0
        for dz in range(4):
            for dc in range(4):
                if dz or dc:
                    copy(part.at[me], part.at[me], p_send.at[index], p_recv.at[0],
                         dev((z + dz) % 4, (col + dc) % 4)).start()
                    index += 1

    def collect(part):
        wait_recv(part.at[pl.ds(0, 15)], p_recv.at[0])
        for index in range(15):
            wait_send(part.at[me], p_send.at[index])
        return jnp.sum(part[...], axis=0)

    copy(h_ref, block_at(z, col), g_send.at[1], g_recv.at[1], ypart).start()
    copy(h_ref, block_at(z, col), g_send.at[2], g_recv.at[2], zpart).start()
    copy(h_ref, block_at(z, col), g_send.at[0], g_recv.at[0], sib).start()
    X[0, own_rows, own_cols] = h_ref[...]
    row_id = lax.broadcasted_iota(jnp.int32, (blk, blk), 0) + z * blk
    col_id = lax.broadcasted_iota(jnp.int32, (blk, blk), 1) + col * blk
    part0[me] = jnp.full((8, 128), jnp.sum(jnp.where(row_id == col_id, h_ref[...], 0.0)), F32)
    share(part0)

    d_pieces = []
    for which in range(2):
        d_pieces.append((which, 0, 1))
        d_pieces.append((which, T, 2))

    def d_rows(which, zz):
        r = (zz + which) % 2
        return pl.ds(pl.multiple_of(r * blk, blk), blk)

    def d_send(which):
        @pl.when(jnp.logical_and(c == 0, inner == 1))
        def _():
            ud = 1 - u
            rows = d_rows(which, z)
            copy(X.at[0, rows, pl.ds(2 * T, T)], D.at[0, rows, pl.ds(0, T)],
                 g_send.at[7 + 2 * which], g_recv.at[7 + 2 * which], dev(opp, sib_col)).start()
            copy(X.at[0, rows, pl.ds(pl.multiple_of(ud * 3 * T, T), 2 * T)], D.at[0, rows, pl.ds(T, 2 * T)],
                 g_send.at[8 + 2 * which], g_recv.at[8 + 2 * which], dev(opp, sib_col)).start()

    wait_recv(block_at(z, yp_col), g_recv.at[1])
    copy(block_at(z, yp_col), block_at(z, yp_col), g_send.at[3], g_recv.at[3], sib).start()
    wait_recv(block_at(z, sib_col), g_recv.at[0])
    wait_recv(block_at(zp, col), g_recv.at[2])
    copy(block_at(zp, col), block_at(zp, col), g_send.at[5], g_recv.at[5], ypart).start()
    copy(block_at(zp, col), block_at(zp, col), g_send.at[4], g_recv.at[4], sib).start()
    wait_recv(block_at(z, sib_yp_col), g_recv.at[3])
    d_send(0)
    wait_recv(block_at(zp, yp_col), g_recv.at[5])
    copy(block_at(zp, yp_col), block_at(zp, yp_col), g_send.at[6], g_recv.at[6], sib).start()
    wait_recv(block_at(zp, sib_col), g_recv.at[4])
    wait_recv(block_at(zp, sib_yp_col), g_recv.at[6])
    d_send(1)
    src_z = 3 - inner_z

    def d_piece(which, first, count):
        return D.at[0, d_rows(which, src_z), pl.ds(first, count * T)]

    @pl.when(c == 1)
    def _():
        for index, (which, first, count) in enumerate(d_pieces):
            wait_recv(d_piece(which, first, count), g_recv.at[7 + index])

            @pl.when(inner == 1)
            def _():
                copy(d_piece(which, first, count), d_piece(which, first, count), g_send.at[7 + index],
                     g_recv.at[7 + index], dev(outer, col)).start()

    total = collect(part0)
    mu = total / order
    occupied = jnp.full((8, 128), count_ref[0], jnp.int32).astype(F32)
    scale = jnp.minimum(occupied / (bounds_ref[1] - mu), (order - occupied) / (mu - bounds_ref[0])) / order
    shift = occupied / order
    mu, scale, shift = mu[0:1, 0:1], scale[0:1, 0:1], shift[0:1, 0:1]

    for index in range(7):
        wait_send(h_ref, g_send.at[index])

    @pl.when(inner == 1)
    def _():
        for index, (which, first, count) in enumerate(d_pieces):
            wait_send(d_piece(which, first, count), g_send.at[7 + index])

    iota_r = lax.broadcasted_iota(jnp.int32, (T, T), 0)
    iota_c = lax.broadcasted_iota(jnp.int32, (T, T), 1)

    def start_tile(tile, slab_r, slab_c):
        diag = iota_r + slab_r * T == iota_c + slab_c * T
        return scale * (jnp.where(diag, mu, 0.0) - tile) + jnp.where(diag, shift, 0.0)

    def start_x(index, carry):
        i, k = index // 10, index % 10
        X[0, ds(i, T), ds(k, T)] = start_tile(X[0, ds(i, T), ds(k, T)], i, k)
        return carry

    lax.fori_loop(0, 50, start_x, 0)

    def set_slab(jj):
        return (2, 3 * u, 3 * u + 1)[jj]

    @pl.when(c == 1)
    def _():
        for jj in range(3):
            def start_d(k, carry):
                D[0, ds(k, T), ds(jj, T)] = start_tile(D[0, ds(k, T), ds(jj, T)], k, set_slab(jj))
                return carry

            lax.fori_loop(0, 5, start_d, 0)

    def split(index, tile):
        first = tile.astype(BF16)
        rest = tile - first.astype(F32)
        second = rest.astype(BF16)
        S[index, 0] = first
        S[index, 1] = second
        S[index, 2] = (rest - second.astype(F32)).astype(BF16)

    def product(left, right, dims):
        acc = None
        for a, b in TERMS:
            for k in range(10):
                term = lax.dot_general(S[left + k, a], S[right + k, b], dims, preferred_element_type=F32)
                acc = term if acc is None else acc + term
        return acc

    def member(label, who):
        return jnp.logical_or(label == 0, label % 2 == 1 - who)

    def x_tile(par, r, k):
        return X.at[par, ds(r, T), ds(k, T)]

    def d_tile(par, r, jj):
        return D.at[par, ds(r, T), ds(jj, T)]

    def d_place(i, s, who):
        in_s = member(s, who)
        return jnp.where(in_s, slab_of(i), slab_of(s)), jnp.where(in_s, (s + 1) // 2, (i + 1) // 2)

    def send0_drain(t):
        par = t % 2

        def stage(s, carry):
            def one(i, carry):
                n = s * (s + 1) // 2 + i
                wait_send(x_tile(0, 0, 0), send.at[par, n])

                @pl.when(i < s)
                def _():
                    wait_send(x_tile(0, 0, 0), send.at[par, 15 + n])

                needed = jnp.logical_or(member(s, 1 - u), member(i, 1 - u))

                @pl.when(jnp.logical_and(jnp.logical_and(inner == 1, t < steps), needed))
                def _():
                    wait_send(x_tile(0, 0, 0), send.at[par, 30 + n])
                return carry
            return lax.fori_loop(0, s + 1, one, carry)

        lax.fori_loop(0, 5, stage, 0)

    def send1_drain(t):
        par = t % 2

        def row(r, carry):
            for jj in range(3):
                wait_send(x_tile(0, 0, 0), send.at[par, 3 * r + jj])
                if jj:
                    wait_send(x_tile(0, 0, 0), send.at[par, 15 + 3 * r + jj])
            for q in range(2):
                wait_send(x_tile(0, 0, 0), send.at[par, 30 + 2 * r + q])

            @pl.when(jnp.logical_and(inner == 1, t < steps))
            def _():
                def one(i, carry):
                    @pl.when(jnp.logical_or(member(r, u), member(i, u)))
                    def _():
                        row_slab, jj = d_place(i, r, u)
                        wait_send(x_tile(0, 0, 0), send.at[par, 40 + 3 * row_slab + jj])
                    return carry
                lax.fori_loop(0, r + 1, one, 0)
            return carry

        lax.fori_loop(0, 5, row, 0)

    def step(t, carry):
        cur, nxt = t % 2, (t + 1) % 2
        flag = flag_ref[t].astype(F32)
        on_square, on_old = 2.0 * flag - 1.0, 2.0 - 2.0 * flag

        @pl.when(c == 0)
        def _():
            @pl.when(t >= 1)
            def _():
                pl.semaphore_wait(credit.at[0], 1)

                @pl.when(jnp.logical_and(inner == 1, t < steps - 1))
                def _():
                    pl.semaphore_wait(credit.at[2], 1)

            def stage(s, carry):
                gs = slab_of(s)

                @pl.when(t >= 1)
                def _():
                    for k in range(5, 10):
                        wait_recv(x_tile(cur, gs, k), recv_x.at[cur, gs * 10 + k])

                def split_one(k, carry):
                    split(s * 10 + k, X[cur, ds(gs, T), ds(k, T)])
                    return carry

                lax.fori_loop(0, 10, split_one, 0)

                def one(i, carry):
                    n = s * (s + 1) // 2 + i
                    gi = slab_of(i)
                    new = on_square * product(i * 10, s * 10, NT) + on_old * X[cur, ds(gi, T), ds(gs, T)]
                    X[nxt, ds(gi, T), ds(gs, T)] = new
                    copy(x_tile(nxt, gi, gs), x_tile(nxt, gi, gs), send.at[nxt, n], recv_x.at[nxt, gi * 10 + gs],
                         sib).start()

                    @pl.when(i < s)
                    def _():
                        X[nxt, ds(gs, T), ds(gi, T)] = X[nxt, ds(gi, T), ds(gs, T)].T
                        copy(x_tile(nxt, gs, gi), x_tile(nxt, gs, gi), send.at[nxt, 15 + n],
                             recv_x.at[nxt, gs * 10 + gi], sib).start()

                    who = 1 - u
                    across = jnp.logical_and(inner == 1, t < steps - 1)

                    @pl.when(jnp.logical_and(across, jnp.logical_or(member(s, who), member(i, who))))
                    def _():
                        row_slab, jj = d_place(i, s, who)
                        in_s = member(s, who)
                        src_r, src_c = jnp.where(in_s, gi, gs), jnp.where(in_s, gs, gi)
                        copy(x_tile(nxt, src_r, src_c), d_tile(nxt, row_slab, jj), send.at[nxt, 30 + n],
                             recv_d.at[nxt, 3 * row_slab + jj], dev(opp, sib_col)).start()
                    return carry

                return lax.fori_loop(0, s + 1, one, carry)

            lax.fori_loop(0, 5, stage, 0)

            @pl.when(t >= 1)
            def _():
                send0_drain(t)

        @pl.when(c == 1)
        def _():
            @pl.when(t >= 1)
            def _():
                pl.semaphore_wait(credit.at[0], 1)
                pl.semaphore_wait(credit.at[1], 1)

                @pl.when(jnp.logical_and(inner == 1, t < steps - 1))
                def _():
                    pl.semaphore_wait(credit.at[2], 1)

                for a, b in ((1, 0), (2, 0), (2, 1)):
                    D[cur, ds(set_slab(a), T), ds(b, T)] = D[cur, ds(set_slab(b), T), ds(a, T)].T

            for jj in range(3):
                def split_o(k, carry):
                    split(jj * 10 + k, X[cur, ds(k, T), ds(5 + set_slab(jj), T)])
                    split(jj * 10 + 5 + k, D[cur, ds(k, T), ds(jj, T)])
                    return carry

                lax.fori_loop(0, 5, split_o, 0)

            def forward(r):
                gr = slab_of(r)
                for q in range(2):
                    k = 5 + 3 * (1 - u) + q
                    wait_recv(x_tile(nxt, gr, k), recv_x.at[nxt, gr * 10 + k])
                    copy(x_tile(nxt, gr, k), x_tile(nxt, gr, k), send.at[nxt, 30 + 2 * r + q],
                         recv_x.at[nxt, gr * 10 + k], sib).start()

                @pl.when(t < steps - 1)
                def _():
                    def one(i, carry):
                        @pl.when(jnp.logical_or(member(r, u), member(i, u)))
                        def _():
                            row_slab, jj = d_place(i, r, u)
                            tile = d_tile(nxt, row_slab, jj)
                            wait_recv(tile, recv_d.at[nxt, 3 * row_slab + jj])

                            @pl.when(inner == 1)
                            def _():
                                copy(tile, tile, send.at[nxt, 40 + 3 * row_slab + jj],
                                     recv_d.at[nxt, 3 * row_slab + jj], dev(outer, col)).start()
                        return carry
                    lax.fori_loop(0, r + 1, one, 0)

            def row(r, carry):
                gr = slab_of(r)

                @pl.when(t >= 1)
                def _():
                    for k in range(5):
                        wait_recv(x_tile(cur, gr, k), recv_x.at[cur, gr * 10 + k])

                def split_one(k, carry):
                    split(30 + k, X[cur, ds(gr, T), ds(k, T)])
                    return carry

                lax.fori_loop(0, 10, split_one, 0)

                def one(jj, carry):
                    k = 5 + 2 * ((2 - jj) // 2) + ((jj + 1) // 2) * (3 * u + jj - 1)
                    new = on_square * product(30, jj * 10, NN) + on_old * X[cur, ds(gr, T), ds(k, T)]
                    X[nxt, ds(gr, T), ds(k, T)] = new
                    copy(x_tile(nxt, gr, k), x_tile(nxt, gr, k), send.at[nxt, 3 * r + jj],
                         recv_x.at[nxt, gr * 10 + k], sib).start()

                    @pl.when(jj > 0)
                    def _():
                        copy(x_tile(nxt, gr, k), x_tile(nxt, gr, k), send.at[nxt, 15 + 3 * r + jj],
                             recv_x.at[nxt, gr * 10 + k], ypart).start()
                    return carry

                lax.fori_loop(0, 3, one, 0)

                @pl.when(r >= 1)
                def _():
                    forward(r - 1)
                return carry

            lax.fori_loop(0, 5, row, 0)
            forward(4)

            @pl.when(t >= 1)
            def _():
                send1_drain(t)

        own = X[cur, own_rows, own_cols]
        line = lax.broadcasted_iota(jnp.int32, (8, 128), 0)
        stats[...] = jnp.where(line == t, jnp.sum(own * own), stats[...])

        @pl.when(t < steps - 1)
        def _():
            pl.semaphore_signal(credit.at[0], inc=1, device_id=sib, device_id_type=MESH)

            @pl.when(c == 1)
            def _():
                pl.semaphore_signal(credit.at[1], inc=1, device_id=ypart, device_id_type=MESH)

                @pl.when(t < steps - 2)
                def _():
                    @pl.when(inner == 1)
                    def _():
                        pl.semaphore_signal(credit.at[2], inc=1, device_id=dev(opp, sib_col), device_id_type=MESH)

                    @pl.when(inner == 0)
                    def _():
                        pl.semaphore_signal(credit.at[2], inc=1, device_id=dev(inner_z, col), device_id_type=MESH)
        return carry

    stats[...] = jnp.zeros_like(stats)
    lax.fori_loop(0, steps, step, 0)
    last = steps % 2

    def last_wait(r, carry):
        for k in range(5):
            where = 5 * (1 - c) + k
            wait_recv(x_tile(last, r, where), recv_x.at[last, r * 10 + where])
        return carry

    lax.fori_loop(0, 5, last_wait, 0)

    final = X[last, own_rows, own_cols]
    out_ref[...] = final
    line = lax.broadcasted_iota(jnp.int32, (8, 128), 0)
    part1[me] = jnp.where(line == steps, jnp.sum(final * h_ref[...]), stats[...])
    share(part1)

    @pl.when(c == 0)
    def _():
        send0_drain(steps)

    @pl.when(c == 1)
    def _():
        send1_drain(steps)

    total = collect(part1)
    for t in range(steps):
        occ_ref[t] = total[t, 0]
    energy_ref[0] = 2.0 * total[steps, 0]


def solution(mesh):
    def local_run(ham_block, bounds, occ_count, branches):
        blk = ham_block.shape[0]
        steps = branches.shape[0]
        T = 2 * blk // 5
        vmem, smem = pl.BlockSpec(memory_space=pltpu.VMEM), pl.BlockSpec(memory_space=pltpu.SMEM)
        return pl.pallas_call(
            functools.partial(kernel, steps),
            out_shape=(jax.ShapeDtypeStruct((blk, blk), F32), jax.ShapeDtypeStruct((steps,), F32),
                       jax.ShapeDtypeStruct((1,), F32)),
            in_specs=[vmem, smem, smem, smem],
            out_specs=(vmem, smem, smem),
            scratch_shapes=[
                pltpu.VMEM((2, 2 * blk, 4 * blk), F32),
                pltpu.VMEM((2, 2 * blk, 3 * T), F32),
                pltpu.VMEM((50, 3, T, T), BF16),
                pltpu.VMEM((8, 128), F32),
                pltpu.VMEM((16, 8, 128), F32),
                pltpu.VMEM((16, 8, 128), F32),
                pltpu.SemaphoreType.DMA((11,)),
                pltpu.SemaphoreType.DMA((11,)),
                pltpu.SemaphoreType.DMA((2, 55)),
                pltpu.SemaphoreType.DMA((2, 50)),
                pltpu.SemaphoreType.DMA((2, 15)),
                pltpu.SemaphoreType.REGULAR((3,)),
                pltpu.SemaphoreType.DMA((15,)),
                pltpu.SemaphoreType.DMA((1,)),
            ],
            compiler_params=pltpu.CompilerParams(collective_id=0, has_side_effects=True, vmem_limit_bytes=67043328),
        )(ham_block, bounds, occ_count, branches)

    return jax.shard_map(local_run, mesh=mesh, in_specs=(P(("spin", "row"), "col"), P("spin"), P("spin"), P("spin")), out_specs=(P(("spin", "row"), "col"), P("spin"), P("spin")), check_vma=False)
```

```python
import functools

import jax
import jax.numpy as jnp
from jax import lax
from jax.experimental import pallas as pl
from jax.experimental.pallas import tpu as pltpu
from jax.sharding import PartitionSpec as P

F32 = jnp.float32
BF16 = jnp.bfloat16
MESH = pl.DeviceIdType.MESH
TERMS = ((0, 2), (2, 0), (1, 1), (0, 1), (1, 0), (0, 0))
NN = (((1,), (0,)), ((), ()))
NT = (((1,), (1,)), ((), ()))


def slab_of(label):
    return label // 2 + 2 * (1 - label % 2)


def kernel(steps, h_ref, bounds_ref, count_ref, flag_ref, out_ref, occ_ref, energy_ref,
           X, D, S, stats, part0, part1, g_send, g_recv, send, recv_x, recv_d, credit, p_send, p_recv):
    blk = h_ref.shape[0]
    T = 2 * blk // 5
    order = 4 * blk
    sid, z, col = lax.axis_index("spin"), lax.axis_index("row"), lax.axis_index("col")
    y, c = col // 2, col % 2
    half = z // 2
    u = (y + half) % 2
    inner = (z + 1) // 2 % 2
    inner = jnp.int32(inner)
    sib_col, yp_col, sib_yp_col = 2 * y + 1 - c, 2 * (1 - y) + c, 2 * (1 - y) + 1 - c
    zp = z + 1 - 2 * (z % 2)
    opp = 3 - z
    outer = 3 * (z // 2)
    inner_z = 1 + half
    me = z * 4 + col

    def dev(zz, cc):
        return (sid, zz, cc)

    sib, ypart, zpart = dev(z, sib_col), dev(z, yp_col), dev(zp, col)

    def copy(src, dst, s_sem, r_sem, device):
        return pltpu.make_async_remote_copy(src_ref=src, dst_ref=dst, send_sem=s_sem, recv_sem=r_sem,
                                            device_id=device, device_id_type=MESH)

    def wait_recv(dst, r_sem):
        copy(dst, dst, g_send.at[0], r_sem, sib).wait_recv()

    def wait_send(src, s_sem):
        copy(src, src, s_sem, g_recv.at[0], sib).wait_send()

    Q = T // 2

    def spans(p):
        return ((3 * p, 0, p * Q, T), (3 * p + 1, 0, p * Q + T, T), (2, p * Q, (1 - p) * 2 * T, Q))

    def at(offset, size):
        return pl.ds(offset if isinstance(offset, int) else pl.multiple_of(offset, Q), size)

    def pieces(zz, cc):
        first = 5 * ((cc // 2 + zz // 2) % 2)
        out = []
        for row, r_in, r_at, r_size in spans(zz % 2):
            for column, c_in, c_at, c_size in spans(cc % 2):
                out.append(((row, first + column, at(r_in, r_size), at(c_in, c_size)),
                            (at(r_at, r_size), at(c_at, c_size))))
        return out

    own = pieces(z, col)

    def send_block(zz, cc, s_sem, r_sem, device, fresh=False):
        for there, here in pieces(zz, cc):
            dst = X.at[(0, *there)]
            copy(h_ref.at[here] if fresh else dst, dst, s_sem, r_sem, device).start()

    barrier = pltpu.get_barrier_semaphore()
    for dz in range(4):
        for dc in range(4):
            if dz or dc:
                pl.semaphore_signal(barrier, inc=1, device_id=dev((z + dz) % 4, (col + dc) % 4), device_id_type=MESH)
    pl.semaphore_wait(barrier, 15)

    def share(part):
        index = 0
        for dz in range(4):
            for dc in range(4):
                if dz or dc:
                    copy(part.at[me], part.at[me], p_send.at[index], p_recv.at[0],
                         dev((z + dz) % 4, (col + dc) % 4)).start()
                    index += 1

    def collect(part):
        wait_recv(part.at[pl.ds(0, 15)], p_recv.at[0])
        for index in range(15):
            wait_send(part.at[me], p_send.at[index])
        return jnp.sum(part[...], axis=0)

    send_block(z, col, g_send.at[1], g_recv.at[1], ypart, True)
    send_block(z, col, g_send.at[2], g_recv.at[2], zpart, True)
    send_block(z, col, g_send.at[0], g_recv.at[0], sib, True)
    for there, here in own:
        X[(0, *there)] = h_ref[here]
    row_id = lax.broadcasted_iota(jnp.int32, (blk, blk), 0) + z * blk
    col_id = lax.broadcasted_iota(jnp.int32, (blk, blk), 1) + col * blk
    part0[me] = jnp.full((8, 128), jnp.sum(jnp.where(row_id == col_id, h_ref[...], 0.0)), F32)
    share(part0)

    def wait_block(r_sem):
        wait_recv(out_ref, r_sem)

    def d_slab(index, zz):
        p = zz % 2
        return (3 * p, 3 * p + 1, 2, 3 * (1 - p), 3 * (1 - p) + 1)[index]

    def set_slab_of(jj, who):
        return (2, 3 * who, 3 * who + 1)[jj]

    def d_send(rows, when):
        @pl.when(jnp.logical_and(jnp.logical_and(c == 0, inner == 1), when))
        def _():
            for index in rows:
                row = d_slab(index, z)
                for jj in range(3):
                    copy(X.at[0, row, set_slab_of(jj, 1 - u)], D.at[0, row, jj], send.at[0, 3 * index + jj],
                         recv_d.at[0, 3 * index + jj], dev(opp, sib_col)).start()

    wait_block(g_recv.at[0])
    d_send((0, 1), u == 0)
    wait_block(g_recv.at[1])
    send_block(z, yp_col, g_send.at[3], g_recv.at[3], sib)
    wait_block(g_recv.at[2])
    send_block(zp, col, g_send.at[5], g_recv.at[5], ypart)
    send_block(zp, col, g_send.at[4], g_recv.at[4], sib)
    wait_block(g_recv.at[3])
    d_send((0, 1), u == 1)
    wait_block(g_recv.at[4])
    d_send((2, 3, 4), u == 0)
    wait_block(g_recv.at[5])
    send_block(zp, yp_col, g_send.at[6], g_recv.at[6], sib)
    wait_block(g_recv.at[6])
    d_send((2, 3, 4), u == 1)

    @pl.when(c == 1)
    def _():
        for index in range(5):
            row = d_slab(index, 3 - inner_z)
            for jj in range(3):
                tile = D.at[0, row, jj]
                wait_recv(tile, recv_d.at[0, 3 * index + jj])

                @pl.when(inner == 1)
                def _():
                    copy(tile, tile, send.at[0, 3 * index + jj], recv_d.at[0, 3 * index + jj], dev(outer, col)).start()

    total = collect(part0)
    mu = total / order
    occupied = jnp.full((8, 128), count_ref[0], jnp.int32).astype(F32)
    scale = jnp.minimum(occupied / (bounds_ref[1] - mu), (order - occupied) / (mu - bounds_ref[0])) / order
    shift = occupied / order
    mu, scale, shift = mu[0:1, 0:1], scale[0:1, 0:1], shift[0:1, 0:1]

    for index in range(7):
        wait_send(out_ref, g_send.at[index])

    @pl.when(inner == 1)
    def _():
        for index in range(15):
            wait_send(D.at[0, 0, 0], send.at[0, index])

    iota_r = lax.broadcasted_iota(jnp.int32, (T, T), 0)
    iota_c = lax.broadcasted_iota(jnp.int32, (T, T), 1)

    def start_tile(tile, slab_r, slab_c):
        diag = iota_r + slab_r * T == iota_c + slab_c * T
        return scale * (jnp.where(diag, mu, 0.0) - tile) + jnp.where(diag, shift, 0.0)

    def start_x(index, carry):
        i, k = index // 10, index % 10
        X[0, i, k] = start_tile(X[0, i, k], i, k)
        return carry

    lax.fori_loop(0, 50, start_x, 0)

    def set_slab(jj):
        return set_slab_of(jj, u)

    @pl.when(c == 1)
    def _():
        for jj in range(3):
            def start_d(k, carry):
                D[0, k, jj] = start_tile(D[0, k, jj], k, set_slab(jj))
                return carry

            lax.fori_loop(0, 5, start_d, 0)

    def split(index, tile):
        first = tile.astype(BF16)
        rest = tile - first.astype(F32)
        second = rest.astype(BF16)
        S[index, 0] = first
        S[index, 1] = second
        S[index, 2] = (rest - second.astype(F32)).astype(BF16)

    def product(left, right, dims):
        acc = None
        for a, b in TERMS:
            for k in range(10):
                term = lax.dot_general(S[left + k, a], S[right + k, b], dims, preferred_element_type=F32)
                acc = term if acc is None else acc + term
        return acc

    def member(label, who):
        return jnp.logical_or(label == 0, label % 2 == 1 - who)

    def x_tile(par, r, k):
        return X.at[par, r, k]

    def d_tile(par, r, jj):
        return D.at[par, r, jj]

    def d_place(i, s, who):
        in_s = member(s, who)
        return jnp.where(in_s, slab_of(i), slab_of(s)), jnp.where(in_s, (s + 1) // 2, (i + 1) // 2)

    def send0_drain(t):
        par = t % 2

        def stage(s, carry):
            def one(i, carry):
                n = s * (s + 1) // 2 + i
                wait_send(x_tile(0, 0, 0), send.at[par, n])

                @pl.when(i < s)
                def _():
                    wait_send(x_tile(0, 0, 0), send.at[par, 15 + n])

                needed = jnp.logical_or(member(s, 1 - u), member(i, 1 - u))

                @pl.when(jnp.logical_and(jnp.logical_and(inner == 1, t < steps), needed))
                def _():
                    wait_send(x_tile(0, 0, 0), send.at[par, 30 + n])
                return carry
            return lax.fori_loop(0, s + 1, one, carry)

        lax.fori_loop(0, 5, stage, 0)

    def send1_drain(t):
        par = t % 2

        def row(r, carry):
            for jj in range(3):
                wait_send(x_tile(0, 0, 0), send.at[par, 3 * r + jj])
                if jj:
                    wait_send(x_tile(0, 0, 0), send.at[par, 15 + 3 * r + jj])
            for q in range(2):
                wait_send(x_tile(0, 0, 0), send.at[par, 30 + 2 * r + q])

            @pl.when(jnp.logical_and(inner == 1, t < steps))
            def _():
                def one(i, carry):
                    @pl.when(jnp.logical_or(member(r, u), member(i, u)))
                    def _():
                        row_slab, jj = d_place(i, r, u)
                        wait_send(x_tile(0, 0, 0), send.at[par, 40 + 3 * row_slab + jj])
                    return carry
                lax.fori_loop(0, r + 1, one, 0)
            return carry

        lax.fori_loop(0, 5, row, 0)

    def forward_x(par, r):
        gr = slab_of(r)
        for q in range(2):
            k = 5 + 3 * (1 - u) + q
            wait_recv(x_tile(par, gr, k), recv_x.at[par, gr * 10 + k])
            copy(x_tile(par, gr, k), x_tile(par, gr, k), send.at[par, 30 + 2 * r + q],
                 recv_x.at[par, gr * 10 + k], sib).start()

    def forward_d(par, s):
        def one(i, carry):
            @pl.when(jnp.logical_or(member(s, u), member(i, u)))
            def _():
                row_slab, jj = d_place(i, s, u)
                tile = d_tile(par, row_slab, jj)
                wait_recv(tile, recv_d.at[par, 3 * row_slab + jj])

                @pl.when(inner == 1)
                def _():
                    copy(tile, tile, send.at[par, 40 + 3 * row_slab + jj],
                         recv_d.at[par, 3 * row_slab + jj], dev(outer, col)).start()
            return carry
        lax.fori_loop(0, s + 1, one, 0)

    def step(t, carry):
        cur, nxt = t % 2, (t + 1) % 2
        flag = flag_ref[t].astype(F32)
        on_square, on_old = 2.0 * flag - 1.0, 2.0 - 2.0 * flag

        @pl.when(c == 0)
        def _():
            def stage(s, carry):
                gs = slab_of(s)

                @pl.when(t >= 1)
                def _():
                    for k in range(5, 10):
                        wait_recv(x_tile(cur, gs, k), recv_x.at[cur, gs * 10 + k])

                def split_one(k, carry):
                    split(s * 10 + k, X[cur, gs, k])
                    return carry

                lax.fori_loop(0, 10, split_one, 0)

                def one(i, carry):
                    n = s * (s + 1) // 2 + i
                    gi = slab_of(i)
                    new = on_square * product(i * 10, s * 10, NT) + on_old * X[cur, gi, gs]
                    X[nxt, gi, gs] = new

                    @pl.when(jnp.logical_and(n == 0, t >= 1))
                    def _():
                        pl.semaphore_wait(credit.at[0], 1)

                        @pl.when(jnp.logical_and(inner == 1, t < steps - 1))
                        def _():
                            pl.semaphore_wait(credit.at[2], 1)

                    copy(x_tile(nxt, gi, gs), x_tile(nxt, gi, gs), send.at[nxt, n], recv_x.at[nxt, gi * 10 + gs],
                         sib).start()

                    @pl.when(i < s)
                    def _():
                        X[nxt, gs, gi] = X[nxt, gi, gs].T
                        copy(x_tile(nxt, gs, gi), x_tile(nxt, gs, gi), send.at[nxt, 15 + n],
                             recv_x.at[nxt, gs * 10 + gi], sib).start()

                    who = 1 - u
                    across = jnp.logical_and(inner == 1, t < steps - 1)

                    @pl.when(jnp.logical_and(across, jnp.logical_or(member(s, who), member(i, who))))
                    def _():
                        row_slab, jj = d_place(i, s, who)
                        in_s = member(s, who)
                        src_r, src_c = jnp.where(in_s, gi, gs), jnp.where(in_s, gs, gi)
                        copy(x_tile(nxt, src_r, src_c), d_tile(nxt, row_slab, jj), send.at[nxt, 30 + n],
                             recv_d.at[nxt, 3 * row_slab + jj], dev(opp, sib_col)).start()
                    return carry

                return lax.fori_loop(0, s + 1, one, carry)

            lax.fori_loop(0, 5, stage, 0)

            @pl.when(t >= 1)
            def _():
                send0_drain(t)

        @pl.when(c == 1)
        def _():
            for jj in range(3):
                def split_o(k, carry):
                    split(jj * 10 + k, X[cur, k, 5 + set_slab(jj)])
                    return carry

                lax.fori_loop(0, 5, split_o, 0)

            @pl.when(t >= 1)
            def _():
                forward_x(cur, 4)
                forward_d(cur, 4)
                for a, b in ((1, 0), (2, 0), (2, 1)):
                    D[cur, set_slab(a), b] = D[cur, set_slab(b), a].T

            for jj in range(3):
                def split_p(k, carry):
                    split(jj * 10 + 5 + k, D[cur, k, jj])
                    return carry

                lax.fori_loop(0, 5, split_p, 0)

            def row(r, carry):
                gr = slab_of(r)

                @pl.when(t >= 1)
                def _():
                    for k in range(5):
                        wait_recv(x_tile(cur, gr, k), recv_x.at[cur, gr * 10 + k])

                def split_one(k, carry):
                    split(30 + k, X[cur, gr, k])
                    return carry

                lax.fori_loop(0, 10, split_one, 0)

                def one(jj, carry):
                    k = 5 + 2 * ((2 - jj) // 2) + ((jj + 1) // 2) * (3 * u + jj - 1)
                    new = on_square * product(30, jj * 10, NN) + on_old * X[cur, gr, k]
                    X[nxt, gr, k] = new

                    @pl.when(jnp.logical_and(jnp.logical_and(r == 0, jj == 0), t >= 1))
                    def _():
                        pl.semaphore_wait(credit.at[0], 1)
                        pl.semaphore_wait(credit.at[1], 1)

                        @pl.when(jnp.logical_and(inner == 1, t < steps - 1))
                        def _():
                            pl.semaphore_wait(credit.at[2], 1)

                    copy(x_tile(nxt, gr, k), x_tile(nxt, gr, k), send.at[nxt, 3 * r + jj],
                         recv_x.at[nxt, gr * 10 + k], sib).start()

                    @pl.when(jj > 0)
                    def _():
                        copy(x_tile(nxt, gr, k), x_tile(nxt, gr, k), send.at[nxt, 15 + 3 * r + jj],
                             recv_x.at[nxt, gr * 10 + k], ypart).start()
                    return carry

                lax.fori_loop(0, 3, one, 0)

                @pl.when(r >= 1)
                def _():
                    forward_x(nxt, r - 1)

                    @pl.when(t < steps - 1)
                    def _():
                        forward_d(nxt, r - 1)
                return carry

            lax.fori_loop(0, 5, row, 0)

            @pl.when(t >= 1)
            def _():
                send1_drain(t)

        line = lax.broadcasted_iota(jnp.int32, (8, 128), 0)
        squares = sum(jnp.sum(jnp.square(X[(cur, *there)])) for there, _ in own)
        stats[...] = jnp.where(line == t, squares, stats[...])

        @pl.when(t < steps - 1)
        def _():
            pl.semaphore_signal(credit.at[0], inc=1, device_id=sib, device_id_type=MESH)

            @pl.when(c == 1)
            def _():
                pl.semaphore_signal(credit.at[1], inc=1, device_id=ypart, device_id_type=MESH)

                @pl.when(t < steps - 2)
                def _():
                    @pl.when(inner == 1)
                    def _():
                        pl.semaphore_signal(credit.at[2], inc=1, device_id=dev(opp, sib_col), device_id_type=MESH)

                    @pl.when(inner == 0)
                    def _():
                        pl.semaphore_signal(credit.at[2], inc=1, device_id=dev(inner_z, col), device_id_type=MESH)
        return carry

    stats[...] = jnp.zeros_like(stats)
    lax.fori_loop(0, steps, step, 0)
    last = steps % 2

    @pl.when(c == 1)
    def _():
        forward_x(last, 4)

    def last_wait(r, carry):
        for k in range(5):
            where = 5 * (1 - c) + k
            wait_recv(x_tile(last, r, where), recv_x.at[last, r * 10 + where])
        return carry

    lax.fori_loop(0, 5, last_wait, 0)

    energy = jnp.float32(0.0)
    for there, here in own:
        final = X[(last, *there)]
        out_ref[here] = final
        energy += jnp.sum(final * h_ref[here])
    line = lax.broadcasted_iota(jnp.int32, (8, 128), 0)
    part1[me] = jnp.where(line == steps, energy, stats[...])
    share(part1)

    @pl.when(c == 0)
    def _():
        send0_drain(steps)

    @pl.when(c == 1)
    def _():
        send1_drain(steps)

    total = collect(part1)
    for t in range(steps):
        occ_ref[t] = total[t, 0]
    energy_ref[0] = 2.0 * total[steps, 0]


def solution(mesh):
    def local_run(ham_block, bounds, occ_count, branches):
        blk = ham_block.shape[0]
        steps = branches.shape[0]
        T = 2 * blk // 5
        vmem, smem = pl.BlockSpec(memory_space=pltpu.VMEM), pl.BlockSpec(memory_space=pltpu.SMEM)
        return pl.pallas_call(
            functools.partial(kernel, steps),
            out_shape=(jax.ShapeDtypeStruct((blk, blk), F32), jax.ShapeDtypeStruct((steps,), F32),
                       jax.ShapeDtypeStruct((1,), F32)),
            in_specs=[vmem, smem, smem, smem],
            out_specs=(vmem, smem, smem),
            scratch_shapes=[
                pltpu.VMEM((2, 5, 10, T, T), F32),
                pltpu.VMEM((2, 5, 3, T, T), F32),
                pltpu.VMEM((50, 3, T, T), BF16),
                pltpu.VMEM((8, 128), F32),
                pltpu.VMEM((16, 8, 128), F32),
                pltpu.VMEM((16, 8, 128), F32),
                pltpu.SemaphoreType.DMA((11,)),
                pltpu.SemaphoreType.DMA((11,)),
                pltpu.SemaphoreType.DMA((2, 55)),
                pltpu.SemaphoreType.DMA((2, 50)),
                pltpu.SemaphoreType.DMA((2, 15)),
                pltpu.SemaphoreType.REGULAR((3,)),
                pltpu.SemaphoreType.DMA((15,)),
                pltpu.SemaphoreType.DMA((1,)),
            ],
            compiler_params=pltpu.CompilerParams(collective_id=0, has_side_effects=True, vmem_limit_bytes=67043328),
        )(ham_block, bounds, occ_count, branches)

    return jax.shard_map(local_run, mesh=mesh, in_specs=(P(("spin", "row"), "col"), P("spin"), P("spin"), P("spin")), out_specs=(P(("spin", "row"), "col"), P("spin"), P("spin")), check_vma=False)
```

```python
import functools

import jax
import jax.numpy as jnp
from jax import lax
from jax.experimental import pallas as pl
from jax.experimental.pallas import tpu as pltpu
from jax.sharding import PartitionSpec as P

F32 = jnp.float32
BF16 = jnp.bfloat16
MESH = pl.DeviceIdType.MESH
TERMS = ((0, 2), (2, 0), (1, 1), (0, 1), (1, 0), (0, 0))
NN = (((1,), (0,)), ((), ()))
NT = (((1,), (1,)), ((), ()))


def slab_of(label):
    return label // 2 + 2 * (1 - label % 2)


def kernel(steps, h_ref, bounds_ref, count_ref, flag_ref, out_ref, occ_ref, energy_ref,
           X, D, S, stats, part0, part1, g_send, g_recv, send, recv_x, recv_d, credit, p_send, p_recv):
    blk = h_ref.shape[0]
    T = 2 * blk // 5
    order = 4 * blk
    sid, z, col = lax.axis_index("spin"), lax.axis_index("row"), lax.axis_index("col")
    y, c = col // 2, col % 2
    half = z // 2
    u = (y + half) % 2
    inner = (z + 1) // 2 % 2
    inner = jnp.int32(inner)
    sib_col, yp_col, sib_yp_col = 2 * y + 1 - c, 2 * (1 - y) + c, 2 * (1 - y) + 1 - c
    zp = z + 1 - 2 * (z % 2)
    opp = 3 - z
    outer = 3 * (z // 2)
    inner_z = 1 + half
    me = z * 4 + col

    def dev(zz, cc):
        return (sid, zz, cc)

    sib, ypart, zpart = dev(z, sib_col), dev(z, yp_col), dev(zp, col)

    def copy(src, dst, s_sem, r_sem, device):
        return pltpu.make_async_remote_copy(src_ref=src, dst_ref=dst, send_sem=s_sem, recv_sem=r_sem,
                                            device_id=device, device_id_type=MESH)

    def wait_recv(dst, r_sem):
        copy(dst, dst, g_send.at[0], r_sem, sib).wait_recv()

    def wait_send(src, s_sem):
        copy(src, src, s_sem, g_recv.at[0], sib).wait_send()

    Q = T // 2

    def spans(p):
        return ((3 * p, 0, p * Q, T), (3 * p + 1, 0, p * Q + T, T), (2, p * Q, (1 - p) * 2 * T, Q))

    def at(offset, size):
        return pl.ds(offset if isinstance(offset, int) else pl.multiple_of(offset, Q), size)

    def pieces(zz, cc):
        first = 5 * ((cc // 2 + zz // 2) % 2)
        out = []
        for row, r_in, r_at, r_size in spans(zz % 2):
            for column, c_in, c_at, c_size in spans(cc % 2):
                out.append(((row, first + column, at(r_in, r_size), at(c_in, c_size)),
                            (at(r_at, r_size), at(c_at, c_size))))
        return out

    own = pieces(z, col)

    def send_block(zz, cc, s_sem, r_sem, device, fresh=False):
        for there, here in pieces(zz, cc):
            dst = X.at[(0, *there)]
            copy(h_ref.at[here] if fresh else dst, dst, s_sem, r_sem, device).start()

    barrier = pltpu.get_barrier_semaphore()
    for dz in range(4):
        for dc in range(4):
            if dz or dc:
                pl.semaphore_signal(barrier, inc=1, device_id=dev((z + dz) % 4, (col + dc) % 4), device_id_type=MESH)
    pl.semaphore_wait(barrier, 15)

    def share(part):
        index = 0
        for dz in range(4):
            for dc in range(4):
                if dz or dc:
                    copy(part.at[me], part.at[me], p_send.at[index], p_recv.at[0],
                         dev((z + dz) % 4, (col + dc) % 4)).start()
                    index += 1

    def collect(part):
        wait_recv(part.at[pl.ds(0, 15)], p_recv.at[0])
        for index in range(15):
            wait_send(part.at[me], p_send.at[index])
        return jnp.sum(part[...], axis=0)

    send_block(z, col, g_send.at[1], g_recv.at[1], ypart, True)
    send_block(z, col, g_send.at[2], g_recv.at[2], zpart, True)
    send_block(z, col, g_send.at[0], g_recv.at[0], sib, True)
    for there, here in own:
        X[(0, *there)] = h_ref[here]
    row_id = lax.broadcasted_iota(jnp.int32, (blk, blk), 0) + z * blk
    col_id = lax.broadcasted_iota(jnp.int32, (blk, blk), 1) + col * blk
    part0[me] = jnp.full((8, 128), jnp.sum(jnp.where(row_id == col_id, h_ref[...], 0.0)), F32)
    share(part0)

    def wait_block(r_sem):
        wait_recv(out_ref, r_sem)

    def d_slab(index, zz):
        p = zz % 2
        return (3 * p, 3 * p + 1, 2, 3 * (1 - p), 3 * (1 - p) + 1)[index]

    def set_slab_of(jj, who):
        return (2, 3 * who, 3 * who + 1)[jj]

    def d_send(rows, when):
        @pl.when(jnp.logical_and(jnp.logical_and(c == 0, inner == 1), when))
        def _():
            for index in rows:
                row = d_slab(index, z)
                for jj in range(3):
                    copy(X.at[0, row, set_slab_of(jj, 1 - u)], D.at[0, row, jj], send.at[0, 3 * index + jj],
                         recv_d.at[0, 3 * index + jj], dev(opp, sib_col)).start()

    def relay(rows, when):
        @pl.when(jnp.logical_and(c == 1, when))
        def _():
            for index in rows:
                row = d_slab(index, 3 - inner_z)
                for jj in range(3):
                    tile = D.at[0, row, jj]
                    wait_recv(tile, recv_d.at[0, 3 * index + jj])

                    @pl.when(inner == 1)
                    def _():
                        copy(tile, tile, send.at[0, 3 * index + jj], recv_d.at[0, 3 * index + jj],
                             dev(outer, col)).start()

    over_y = jnp.logical_or(inner == 0, c == 0)
    over_z = jnp.logical_and(inner == 0, c == 1)
    wait_block(g_recv.at[0])
    d_send((0, 1), u == 0)
    wait_block(g_recv.at[1])

    @pl.when(over_z)
    def _():
        send_block(z, yp_col, g_send.at[7], g_recv.at[5], zpart)

    send_block(z, yp_col, g_send.at[3], g_recv.at[3], sib)
    wait_block(g_recv.at[2])

    @pl.when(over_y)
    def _():
        send_block(zp, col, g_send.at[5], g_recv.at[5], ypart)

    send_block(zp, col, g_send.at[4], g_recv.at[4], sib)
    wait_block(g_recv.at[3])
    d_send((0, 1), u == 1)
    wait_block(g_recv.at[4])
    d_send((2, 3, 4), u == 0)
    early = jnp.logical_and(inner == 1, u == 1)
    relay((0, 1), early)
    wait_block(g_recv.at[5])
    send_block(zp, yp_col, g_send.at[6], g_recv.at[6], sib)
    wait_block(g_recv.at[6])
    d_send((2, 3, 4), u == 1)

    total = collect(part0)
    mu = total / order
    occupied = jnp.full((8, 128), count_ref[0], jnp.int32).astype(F32)
    scale = jnp.minimum(occupied / (bounds_ref[1] - mu), (order - occupied) / (mu - bounds_ref[0])) / order
    shift = occupied / order
    mu, scale, shift = mu[0:1, 0:1], scale[0:1, 0:1], shift[0:1, 0:1]

    iota_r = lax.broadcasted_iota(jnp.int32, (T, T), 0)
    iota_c = lax.broadcasted_iota(jnp.int32, (T, T), 1)

    def start_tile(tile, slab_r, slab_c):
        diag = iota_r + slab_r * T == iota_c + slab_c * T
        return scale * (jnp.where(diag, mu, 0.0) - tile) + jnp.where(diag, shift, 0.0)

    def set_slab(jj):
        return set_slab_of(jj, u)

    relay((0, 1), jnp.logical_not(early))
    relay((2, 3, 4), c == 1)

    first_on = -scale
    first_diag = scale * mu + shift

    def old_tile(t, tile, slab_r, slab_c):
        diag = iota_r + slab_r * T == iota_c + slab_c * T
        first = (t == 0).astype(jnp.int32).astype(F32)
        keep = 1.0 - first
        return (first * first_on + keep) * tile + jnp.where(diag, first * first_diag, 0.0)

    def split_first(t, index, tile, slab_r, slab_c):
        @pl.when(t == 0)
        def _():
            split(index, start_tile(tile, slab_r, slab_c))

        @pl.when(t > 0)
        def _():
            split(index, tile)

    def split(index, tile):
        first = tile.astype(BF16)
        rest = tile - first.astype(F32)
        second = rest.astype(BF16)
        S[index, 0] = first
        S[index, 1] = second
        S[index, 2] = (rest - second.astype(F32)).astype(BF16)

    def product(left, right, dims):
        acc = None
        for a, b in TERMS:
            for k in range(10):
                term = lax.dot_general(S[left + k, a], S[right + k, b], dims, preferred_element_type=F32)
                acc = term if acc is None else acc + term
        return acc

    def member(label, who):
        return jnp.logical_or(label == 0, label % 2 == 1 - who)

    def x_tile(par, r, k):
        return X.at[par, r, k]

    def d_tile(par, r, jj):
        return D.at[par, r, jj]

    def d_place(i, s, who):
        in_s = member(s, who)
        return jnp.where(in_s, slab_of(i), slab_of(s)), jnp.where(in_s, (s + 1) // 2, (i + 1) // 2)

    def send0_drain(t):
        par = t % 2

        def stage(s, carry):
            def one(i, carry):
                n = s * (s + 1) // 2 + i
                wait_send(x_tile(0, 0, 0), send.at[par, n])

                @pl.when(i < s)
                def _():
                    wait_send(x_tile(0, 0, 0), send.at[par, 15 + n])

                needed = jnp.logical_or(member(s, 1 - u), member(i, 1 - u))

                @pl.when(jnp.logical_and(jnp.logical_and(inner == 1, t < steps), needed))
                def _():
                    wait_send(x_tile(0, 0, 0), send.at[par, 30 + n])
                return carry
            return lax.fori_loop(0, s + 1, one, carry)

        lax.fori_loop(0, 5, stage, 0)

    def send1_drain(t):
        par = t % 2

        def row(r, carry):
            for jj in range(3):
                wait_send(x_tile(0, 0, 0), send.at[par, 3 * r + jj])
                if jj:
                    wait_send(x_tile(0, 0, 0), send.at[par, 15 + 3 * r + jj])
            for q in range(2):
                wait_send(x_tile(0, 0, 0), send.at[par, 30 + 2 * r + q])

            @pl.when(jnp.logical_and(inner == 1, t < steps))
            def _():
                def one(i, carry):
                    @pl.when(jnp.logical_or(member(r, u), member(i, u)))
                    def _():
                        row_slab, jj = d_place(i, r, u)
                        wait_send(x_tile(0, 0, 0), send.at[par, 40 + 3 * row_slab + jj])
                    return carry
                lax.fori_loop(0, r + 1, one, 0)
            return carry

        lax.fori_loop(0, 5, row, 0)

    def forward_x(par, r):
        gr = slab_of(r)
        for q in range(2):
            k = 5 + 3 * (1 - u) + q
            wait_recv(x_tile(par, gr, k), recv_x.at[par, gr * 10 + k])
            copy(x_tile(par, gr, k), x_tile(par, gr, k), send.at[par, 30 + 2 * r + q],
                 recv_x.at[par, gr * 10 + k], sib).start()

    def forward_d(par, s):
        def one(i, carry):
            @pl.when(jnp.logical_or(member(s, u), member(i, u)))
            def _():
                row_slab, jj = d_place(i, s, u)
                tile = d_tile(par, row_slab, jj)
                wait_recv(tile, recv_d.at[par, 3 * row_slab + jj])

                @pl.when(inner == 1)
                def _():
                    copy(tile, tile, send.at[par, 40 + 3 * row_slab + jj],
                         recv_d.at[par, 3 * row_slab + jj], dev(outer, col)).start()
            return carry
        lax.fori_loop(0, s + 1, one, 0)

    def send_tile(t, nxt, s, i):
        n = s * (s + 1) // 2 + i
        gs, gi = slab_of(s), slab_of(i)
        s, i = jnp.int32(s), jnp.int32(i)
        who = 1 - u
        in_s = member(s, who)

        @pl.when(jnp.logical_and(jnp.logical_and(inner == 1, t < steps - 1), jnp.logical_or(in_s, member(i, who))))
        def _():
            row_slab, jj = d_place(i, s, who)
            src_r, src_c = jnp.where(in_s, gi, gs), jnp.where(in_s, gs, gi)
            copy(x_tile(nxt, src_r, src_c), d_tile(nxt, row_slab, jj), send.at[nxt, 30 + n],
                 recv_d.at[nxt, 3 * row_slab + jj], dev(opp, sib_col)).start()

        copy(x_tile(nxt, gi, gs), x_tile(nxt, gi, gs), send.at[nxt, n], recv_x.at[nxt, gi * 10 + gs], sib).start()

        @pl.when(i < s)
        def _():
            copy(x_tile(nxt, gs, gi), x_tile(nxt, gs, gi), send.at[nxt, 15 + n], recv_x.at[nxt, gs * 10 + gi],
                 sib).start()

    def step(t, carry):
        cur, nxt = t % 2, (t + 1) % 2
        flag = flag_ref[t].astype(F32)
        on_square, on_old = 2.0 * flag - 1.0, 2.0 - 2.0 * flag

        @pl.when(c == 0)
        def _():
            def stage(s, carry):
                gs = slab_of(s)

                @pl.when(t >= 1)
                def _():
                    for k in range(5, 10):
                        wait_recv(x_tile(cur, gs, k), recv_x.at[cur, gs * 10 + k])

                def split_one(k, carry):
                    split_first(t, s * 10 + k, X[cur, gs, k], gs, k)
                    return carry

                lax.fori_loop(0, 10, split_one, 0)

                def one(i, carry):
                    n = s * (s + 1) // 2 + i
                    gi = slab_of(i)
                    new = on_square * product(i * 10, s * 10, NT) + on_old * old_tile(t, X[cur, gi, gs], gi, gs)
                    X[nxt, gi, gs] = new

                    @pl.when(i < s)
                    def _():
                        X[nxt, gs, gi] = X[nxt, gi, gs].T

                    @pl.when(jnp.logical_and(n == 2, t >= 1))
                    def _():
                        pl.semaphore_wait(credit.at[0], 1)

                        @pl.when(jnp.logical_and(inner == 1, t < steps - 1))
                        def _():
                            pl.semaphore_wait(credit.at[2], 1)

                    @pl.when(n == 2)
                    def _():
                        send_tile(t, nxt, 0, 0)
                        send_tile(t, nxt, 1, 0)

                    @pl.when(n >= 2)
                    def _():
                        send_tile(t, nxt, s, i)
                    return carry

                return lax.fori_loop(0, s + 1, one, carry)

            lax.fori_loop(0, 5, stage, 0)

            @pl.when(t >= 1)
            def _():
                send0_drain(t)

        @pl.when(c == 1)
        def _():
            for jj in range(3):
                def split_o(k, carry):
                    split_first(t, jj * 10 + k, X[cur, k, 5 + set_slab(jj)], k, 5 + set_slab(jj))
                    return carry

                lax.fori_loop(0, 5, split_o, 0)

            @pl.when(t >= 1)
            def _():
                forward_x(cur, 4)
                forward_d(cur, 4)
                for a, b in ((1, 0), (2, 0), (2, 1)):
                    D[cur, set_slab(a), b] = D[cur, set_slab(b), a].T

            for jj in range(3):
                def split_p(k, carry):
                    split_first(t, jj * 10 + 5 + k, D[cur, k, jj], k, set_slab(jj))
                    return carry

                lax.fori_loop(0, 5, split_p, 0)

            def row(r, carry):
                gr = slab_of(r)

                @pl.when(t >= 1)
                def _():
                    for k in range(5):
                        wait_recv(x_tile(cur, gr, k), recv_x.at[cur, gr * 10 + k])

                def split_one(k, carry):
                    split_first(t, 30 + k, X[cur, gr, k], gr, k)
                    return carry

                lax.fori_loop(0, 10, split_one, 0)

                def one(jj, carry):
                    k = 5 + 2 * ((2 - jj) // 2) + ((jj + 1) // 2) * (3 * u + jj - 1)
                    new = on_square * product(30, jj * 10, NN) + on_old * old_tile(t, X[cur, gr, k], gr, k)
                    X[nxt, gr, k] = new

                    @pl.when(jnp.logical_and(jnp.logical_and(r == 0, jj == 0), t >= 1))
                    def _():
                        pl.semaphore_wait(credit.at[0], 1)
                        pl.semaphore_wait(credit.at[1], 1)

                        @pl.when(jnp.logical_and(inner == 1, t < steps - 1))
                        def _():
                            pl.semaphore_wait(credit.at[2], 1)

                    copy(x_tile(nxt, gr, k), x_tile(nxt, gr, k), send.at[nxt, 3 * r + jj],
                         recv_x.at[nxt, gr * 10 + k], sib).start()

                    @pl.when(jj > 0)
                    def _():
                        copy(x_tile(nxt, gr, k), x_tile(nxt, gr, k), send.at[nxt, 15 + 3 * r + jj],
                             recv_x.at[nxt, gr * 10 + k], ypart).start()
                    return carry

                lax.fori_loop(0, 3, one, 0)

                @pl.when(r >= 1)
                def _():
                    forward_x(nxt, r - 1)

                    @pl.when(t < steps - 1)
                    def _():
                        forward_d(nxt, r - 1)
                return carry

            lax.fori_loop(0, 5, row, 0)

            @pl.when(t >= 1)
            def _():
                send1_drain(t)

        line = lax.broadcasted_iota(jnp.int32, (8, 128), 0)
        squares = sum(jnp.sum(jnp.square(X[(cur, *there)])) for there, _ in own)

        @pl.when(t > 0)
        def _():
            stats[...] = jnp.where(line == t, squares, stats[...])

        @pl.when(t == 0)
        def _():
            start = scale * (jnp.where(row_id == col_id, mu, 0.0) - h_ref[...]) + jnp.where(row_id == col_id, shift, 0.0)
            stats[...] = jnp.where(line == 0, jnp.sum(start * start), stats[...])
            for index in (0, 1, 2, 3, 4, 6):
                wait_send(out_ref, g_send.at[index])

            @pl.when(over_y)
            def _():
                wait_send(out_ref, g_send.at[5])

            @pl.when(over_z)
            def _():
                wait_send(out_ref, g_send.at[7])

            @pl.when(inner == 1)
            def _():
                for index in range(15):
                    wait_send(D.at[0, 0, 0], send.at[0, index])

        @pl.when(t < steps - 1)
        def _():
            pl.semaphore_signal(credit.at[0], inc=1, device_id=sib, device_id_type=MESH)

            @pl.when(c == 1)
            def _():
                pl.semaphore_signal(credit.at[1], inc=1, device_id=ypart, device_id_type=MESH)

                @pl.when(t < steps - 2)
                def _():
                    @pl.when(inner == 1)
                    def _():
                        pl.semaphore_signal(credit.at[2], inc=1, device_id=dev(opp, sib_col), device_id_type=MESH)

                    @pl.when(inner == 0)
                    def _():
                        pl.semaphore_signal(credit.at[2], inc=1, device_id=dev(inner_z, col), device_id_type=MESH)
        return carry

    stats[...] = jnp.zeros_like(stats)
    lax.fori_loop(0, steps, step, 0)
    last = steps % 2

    @pl.when(c == 1)
    def _():
        forward_x(last, 4)

    def last_wait(r, carry):
        for k in range(5):
            where = 5 * (1 - c) + k
            wait_recv(x_tile(last, r, where), recv_x.at[last, r * 10 + where])
        return carry

    lax.fori_loop(0, 5, last_wait, 0)

    energy = jnp.float32(0.0)
    for there, here in own:
        final = X[(last, *there)]
        out_ref[here] = final
        energy += jnp.sum(final * h_ref[here])
    line = lax.broadcasted_iota(jnp.int32, (8, 128), 0)
    part1[me] = jnp.where(line == steps, energy, stats[...])
    share(part1)

    @pl.when(c == 0)
    def _():
        send0_drain(steps)

    @pl.when(c == 1)
    def _():
        send1_drain(steps)

    total = collect(part1)
    for t in range(steps):
        occ_ref[t] = total[t, 0]
    energy_ref[0] = 2.0 * total[steps, 0]


def solution(mesh):
    def local_run(ham_block, bounds, occ_count, branches):
        blk = ham_block.shape[0]
        steps = branches.shape[0]
        T = 2 * blk // 5
        vmem, smem = pl.BlockSpec(memory_space=pltpu.VMEM), pl.BlockSpec(memory_space=pltpu.SMEM)
        return pl.pallas_call(
            functools.partial(kernel, steps),
            out_shape=(jax.ShapeDtypeStruct((blk, blk), F32), jax.ShapeDtypeStruct((steps,), F32),
                       jax.ShapeDtypeStruct((1,), F32)),
            in_specs=[vmem, smem, smem, smem],
            out_specs=(vmem, smem, smem),
            scratch_shapes=[
                pltpu.VMEM((2, 5, 10, T, T), F32),
                pltpu.VMEM((2, 5, 3, T, T), F32),
                pltpu.VMEM((50, 3, T, T), BF16),
                pltpu.VMEM((8, 128), F32),
                pltpu.VMEM((16, 8, 128), F32),
                pltpu.VMEM((16, 8, 128), F32),
                pltpu.SemaphoreType.DMA((11,)),
                pltpu.SemaphoreType.DMA((11,)),
                pltpu.SemaphoreType.DMA((2, 55)),
                pltpu.SemaphoreType.DMA((2, 50)),
                pltpu.SemaphoreType.DMA((2, 15)),
                pltpu.SemaphoreType.REGULAR((3,)),
                pltpu.SemaphoreType.DMA((15,)),
                pltpu.SemaphoreType.DMA((1,)),
            ],
            compiler_params=pltpu.CompilerParams(collective_id=0, has_side_effects=True, vmem_limit_bytes=67043328),
        )(ham_block, bounds, occ_count, branches)

    return jax.shard_map(local_run, mesh=mesh, in_specs=(P(("spin", "row"), "col"), P("spin"), P("spin"), P("spin")), out_specs=(P(("spin", "row"), "col"), P("spin"), P("spin")), check_vma=False)
```

```python
import functools

import jax
import jax.numpy as jnp
from jax import lax
from jax.experimental import pallas as pl
from jax.experimental.pallas import tpu as pltpu
from jax.sharding import PartitionSpec as P

F32 = jnp.float32
BF16 = jnp.bfloat16
MESH = pl.DeviceIdType.MESH
TERMS = ((0, 2), (2, 0), (1, 1), (0, 1), (1, 0), (0, 0))
NN = (((1,), (0,)), ((), ()))
NT = (((1,), (1,)), ((), ()))


def slab_of(label):
    return label // 2 + 2 * (1 - label % 2)


def kernel(steps, h_ref, bounds_ref, count_ref, flag_ref, out_ref, occ_ref, energy_ref,
           X, D, S, stats, part0, part1, g_send, g_recv, send, recv_x, recv_y, recv_d, credit, p_send, p_recv):
    blk = h_ref.shape[0]
    T = 2 * blk // 5
    order = 4 * blk
    sid, z, col = lax.axis_index("spin"), lax.axis_index("row"), lax.axis_index("col")
    y, c = col // 2, col % 2
    half = z // 2
    u = (y + half) % 2
    inner = (z + 1) // 2 % 2
    inner = jnp.int32(inner)
    sib_col, yp_col, sib_yp_col = 2 * y + 1 - c, 2 * (1 - y) + c, 2 * (1 - y) + 1 - c
    zp = z + 1 - 2 * (z % 2)
    opp = 3 - z
    outer = 3 * (z // 2)
    inner_z = 1 + half
    me = z * 4 + col

    def dev(zz, cc):
        return (sid, zz, cc)

    sib, ypart, zpart = dev(z, sib_col), dev(z, yp_col), dev(zp, col)

    def copy(src, dst, s_sem, r_sem, device):
        return pltpu.make_async_remote_copy(src_ref=src, dst_ref=dst, send_sem=s_sem, recv_sem=r_sem,
                                            device_id=device, device_id_type=MESH)

    def wait_recv(dst, r_sem):
        copy(dst, dst, g_send.at[0], r_sem, sib).wait_recv()

    def wait_send(src, s_sem):
        copy(src, src, s_sem, g_recv.at[0], sib).wait_send()

    Q = T // 2

    def spans(p):
        return ((3 * p, 0, p * Q, T), (3 * p + 1, 0, p * Q + T, T), (2, p * Q, (1 - p) * 2 * T, Q))

    def at(offset, size):
        return pl.ds(offset if isinstance(offset, int) else pl.multiple_of(offset, Q), size)

    def pieces(zz, cc):
        first = 5 * ((cc // 2 + zz // 2) % 2)
        out = []
        for row, r_in, r_at, r_size in spans(zz % 2):
            for column, c_in, c_at, c_size in spans(cc % 2):
                out.append(((row, first + column, at(r_in, r_size), at(c_in, c_size)),
                            (at(r_at, r_size), at(c_at, c_size))))
        return out

    own = pieces(z, col)

    def send_block(zz, cc, s_sem, r_sem, device, fresh=False):
        for there, here in pieces(zz, cc):
            dst = X.at[(0, *there)]
            copy(h_ref.at[here] if fresh else dst, dst, s_sem, r_sem, device).start()

    barrier = pltpu.get_barrier_semaphore()
    for dz in range(4):
        for dc in range(4):
            if dz or dc:
                pl.semaphore_signal(barrier, inc=1, device_id=dev((z + dz) % 4, (col + dc) % 4), device_id_type=MESH)
    pl.semaphore_wait(barrier, 15)

    def share(part):
        index = 0
        for dz in range(4):
            for dc in range(4):
                if dz or dc:
                    copy(part.at[me], part.at[me], p_send.at[index], p_recv.at[0],
                         dev((z + dz) % 4, (col + dc) % 4)).start()
                    index += 1

    def collect(part):
        wait_recv(part.at[pl.ds(0, 15)], p_recv.at[0])
        for index in range(15):
            wait_send(part.at[me], p_send.at[index])
        return jnp.sum(part[...], axis=0)

    send_block(z, col, g_send.at[1], g_recv.at[1], ypart, True)
    send_block(z, col, g_send.at[2], g_recv.at[2], zpart, True)
    send_block(z, col, g_send.at[0], g_recv.at[0], sib, True)
    for there, here in own:
        X[(0, *there)] = h_ref[here]
    row_id = lax.broadcasted_iota(jnp.int32, (blk, blk), 0) + z * blk
    col_id = lax.broadcasted_iota(jnp.int32, (blk, blk), 1) + col * blk
    part0[me] = jnp.full((8, 128), jnp.sum(jnp.where(row_id == col_id, h_ref[...], 0.0)), F32)
    share(part0)

    def wait_block(r_sem):
        wait_recv(out_ref, r_sem)

    def d_slab(index, zz):
        p = zz % 2
        return (3 * p, 3 * p + 1, 2, 3 * (1 - p), 3 * (1 - p) + 1)[index]

    def set_slab_of(jj, who):
        return (2, 3 * who, 3 * who + 1)[jj]

    def d_send(rows, when):
        @pl.when(jnp.logical_and(jnp.logical_and(c == 0, inner == 1), when))
        def _():
            for index in rows:
                row = d_slab(index, z)
                for jj in range(3):
                    copy(X.at[0, row, set_slab_of(jj, 1 - u)], D.at[0, row, jj], g_send.at[8],
                         recv_d.at[0, 3 * index + jj], dev(opp, sib_col)).start()

    def relay(rows, when):
        @pl.when(jnp.logical_and(c == 1, when))
        def _():
            for index in rows:
                row = d_slab(index, 3 - inner_z)
                for jj in range(3):
                    tile = D.at[0, row, jj]
                    wait_recv(tile, recv_d.at[0, 3 * index + jj])

                    @pl.when(inner == 1)
                    def _():
                        copy(tile, tile, g_send.at[8], recv_d.at[0, 3 * index + jj], dev(outer, col)).start()

    over_y = jnp.logical_or(inner == 0, c == 0)
    over_z = jnp.logical_and(inner == 0, c == 1)
    wait_block(g_recv.at[0])
    d_send((0, 1), u == 0)
    wait_block(g_recv.at[1])

    @pl.when(over_z)
    def _():
        send_block(z, yp_col, g_send.at[7], g_recv.at[5], zpart)

    send_block(z, yp_col, g_send.at[3], g_recv.at[3], sib)
    wait_block(g_recv.at[2])

    @pl.when(over_y)
    def _():
        send_block(zp, col, g_send.at[5], g_recv.at[5], ypart)

    send_block(zp, col, g_send.at[4], g_recv.at[4], sib)
    wait_block(g_recv.at[3])
    d_send((0, 1), u == 1)
    wait_block(g_recv.at[4])
    d_send((2, 3, 4), u == 0)
    early = jnp.logical_and(inner == 1, u == 1)
    relay((0, 1), early)
    wait_block(g_recv.at[5])
    send_block(zp, yp_col, g_send.at[6], g_recv.at[6], sib)
    wait_block(g_recv.at[6])
    d_send((2, 3, 4), u == 1)

    total = collect(part0)
    mu = total / order
    occupied = jnp.full((8, 128), count_ref[0], jnp.int32).astype(F32)
    scale = jnp.minimum(occupied / (bounds_ref[1] - mu), (order - occupied) / (mu - bounds_ref[0])) / order
    shift = occupied / order
    mu, scale, shift = mu[0:1, 0:1], scale[0:1, 0:1], shift[0:1, 0:1]

    iota_r = lax.broadcasted_iota(jnp.int32, (T, T), 0)
    iota_c = lax.broadcasted_iota(jnp.int32, (T, T), 1)

    def start_tile(tile, slab_r, slab_c):
        diag = iota_r + slab_r * T == iota_c + slab_c * T
        return scale * (jnp.where(diag, mu, 0.0) - tile) + jnp.where(diag, shift, 0.0)

    def set_slab(jj):
        return set_slab_of(jj, u)

    relay((0, 1), jnp.logical_not(early))
    relay((2, 3, 4), c == 1)

    first_on = -scale
    first_diag = scale * mu + shift

    def old_tile(t, tile, slab_r, slab_c):
        diag = iota_r + slab_r * T == iota_c + slab_c * T
        first = (t == 0).astype(jnp.int32).astype(F32)
        keep = 1.0 - first
        return (first * first_on + keep) * tile + jnp.where(diag, first * first_diag, 0.0)

    def split_first(t, index, tile, slab_r, slab_c):
        @pl.when(t == 0)
        def _():
            split(index, start_tile(tile, slab_r, slab_c))

        @pl.when(t > 0)
        def _():
            split(index, tile)

    def split(index, tile):
        first = tile.astype(BF16)
        rest = tile - first.astype(F32)
        second = rest.astype(BF16)
        S[index, 0] = first
        S[index, 1] = second
        S[index, 2] = (rest - second.astype(F32)).astype(BF16)

    def product(left, right, dims):
        acc = None
        for a, b in TERMS:
            for k in range(10):
                term = lax.dot_general(S[left + k, a], S[right + k, b], dims, preferred_element_type=F32)
                acc = term if acc is None else acc + term
        return acc

    def member(label, who):
        return jnp.logical_or(jnp.int32(label) == 0, label % 2 == 1 - who)

    def x_tile(par, r, k):
        return X.at[par, r, k]

    def d_tile(par, r, jj):
        return D.at[par, r, jj]

    def d_place(i, s, who):
        in_s = member(s, who)
        return jnp.where(in_s, slab_of(i), slab_of(s)), jnp.where(in_s, (s + 1) // 2, (i + 1) // 2)

    fifteen, twelve, ten, nine, six = (D.at[0], X.at[0, pl.ds(0, 4), pl.ds(0, 3)], X.at[0, 0],
                                       X.at[0, pl.ds(0, 3), pl.ds(0, 3)], X.at[0, pl.ds(0, 2), pl.ds(0, 3)])
    plane = z % 2

    def send0_drain(par):
        wait_send(fifteen, send.at[par, 0])
        wait_send(ten, send.at[par, 1])

        @pl.when(inner == 1)
        def _():
            wait_send(twelve, send.at[par, 2])

    def send1_drain(par):
        wait_send(fifteen, send.at[par, 0])
        wait_send(ten, send.at[par, 1])
        wait_send(ten, send.at[par, 3])

        @pl.when(inner == 1)
        def _():
            wait_send(twelve, send.at[par, 2])

    def forward_x(par, r):
        gr = slab_of(r)
        first = 5 + 3 * (1 - u)
        wait_recv(X.at[par, gr, pl.ds(first, 2)], recv_y.at[par, gr])
        for q in range(2):
            tile = x_tile(par, gr, first + q)
            copy(tile, tile, send.at[par, 3], recv_x.at[par, gr], sib).start()

    def forward_d(par, s):
        def one(i, carry):
            @pl.when(jnp.logical_or(member(s, u), member(i, u)))
            def _():
                row_slab, jj = d_place(i, s, u)
                tile = d_tile(par, row_slab, jj)
                wait_recv(tile, recv_d.at[par, 3 * row_slab + jj])

                @pl.when(inner == 1)
                def _():
                    copy(tile, tile, send.at[par, 2],
                         recv_d.at[par, 3 * row_slab + jj], dev(outer, col)).start()
            return carry
        lax.fori_loop(0, s + 1, one, 0)

    def send_tile(t, nxt, s, i):
        gs, gi = slab_of(s), slab_of(i)
        s, i = jnp.int32(s), jnp.int32(i)
        who = 1 - u
        in_s = member(s, who)

        @pl.when(jnp.logical_and(jnp.logical_and(inner == 1, t < steps - 1), jnp.logical_or(in_s, member(i, who))))
        def _():
            row_slab, jj = d_place(i, s, who)
            src_r, src_c = jnp.where(in_s, gi, gs), jnp.where(in_s, gs, gi)
            copy(x_tile(nxt, src_r, src_c), d_tile(nxt, row_slab, jj), send.at[nxt, 2],
                 recv_d.at[nxt, 3 * row_slab + jj], dev(opp, sib_col)).start()

        copy(x_tile(nxt, gi, gs), x_tile(nxt, gi, gs), send.at[nxt, 0], recv_x.at[nxt, gi], sib).start()

        @pl.when(i < s)
        def _():
            copy(x_tile(nxt, gs, gi), x_tile(nxt, gs, gi), send.at[nxt, 1], recv_x.at[nxt, gs], sib).start()

    def step(t, carry):
        cur, nxt = t % 2, (t + 1) % 2
        flag = flag_ref[t].astype(F32)
        on_square, on_old = 2.0 * flag - 1.0, 2.0 - 2.0 * flag

        @pl.when(c == 0)
        def _():
            def stage(s, carry):
                gs = slab_of(s)

                @pl.when(t >= 1)
                def _():
                    wait_recv(X.at[cur, gs, pl.ds(5, 5)], recv_x.at[cur, gs])

                def split_one(k, carry):
                    split_first(t, s * 10 + k, X[cur, gs, k], gs, k)
                    return carry

                lax.fori_loop(0, 10, split_one, 0)

                def one(i, carry):
                    gi = slab_of(i)
                    new = on_square * product(i * 10, s * 10, NT) + on_old * old_tile(t, X[cur, gi, gs], gi, gs)
                    X[nxt, gi, gs] = new

                    @pl.when(i < s)
                    def _():
                        X[nxt, gs, gi] = X[nxt, gi, gs].T

                    return carry

                def needed(i, carry):
                    full = t < steps - 1
                    mine = jnp.logical_and(u == 0, jnp.logical_or(member(i, plane), member(s, plane)))

                    @pl.when(jnp.logical_or(full, mine))
                    def _():
                        one(i, carry)

                    @pl.when(s * (s + 1) // 2 + i == 2)
                    def _():
                        @pl.when(t >= 1)
                        def _():
                            pl.semaphore_wait(credit.at[0], 1)

                            @pl.when(jnp.logical_and(inner == 1, full))
                            def _():
                                pl.semaphore_wait(credit.at[2], 1)

                        @pl.when(jnp.logical_or(full, u == 0))
                        def _():
                            send_tile(t, nxt, 0, 0)
                            send_tile(t, nxt, 1, 0)

                    @pl.when(jnp.logical_and(s * (s + 1) // 2 + i >= 2, jnp.logical_or(full, mine)))
                    def _():
                        send_tile(t, nxt, s, i)
                    return carry

                return lax.fori_loop(0, s + 1, needed, carry)

            lax.fori_loop(0, 5, stage, 0)

            @pl.when(t >= 1)
            def _():
                send0_drain(cur)

        @pl.when(c == 1)
        def _():
            for jj in range(3):
                def split_o(k, carry):
                    split_first(t, jj * 10 + k, X[cur, k, 5 + set_slab(jj)], k, 5 + set_slab(jj))
                    return carry

                lax.fori_loop(0, 5, split_o, 0)

            @pl.when(t >= 1)
            def _():
                forward_x(cur, 4)
                forward_d(cur, 4)
                for a, b in ((1, 0), (2, 0), (2, 1)):
                    D[cur, set_slab(a), b] = D[cur, set_slab(b), a].T

            for jj in range(3):
                def split_p(k, carry):
                    split_first(t, jj * 10 + 5 + k, D[cur, k, jj], k, set_slab(jj))
                    return carry

                lax.fori_loop(0, 5, split_p, 0)

            def row(r, carry):
                gr = slab_of(r)

                @pl.when(t >= 1)
                def _():
                    wait_recv(X.at[cur, gr, pl.ds(0, 5)], recv_x.at[cur, gr])

                @pl.when(jnp.logical_or(t < steps - 1, member(r, plane)))
                def _():
                    active_row(r, gr)

                @pl.when(jnp.logical_and(r >= 1, jnp.logical_or(t < steps - 1, member(r - 1, plane))))
                def _():
                    forward_x(nxt, r - 1)

                    @pl.when(t < steps - 1)
                    def _():
                        forward_d(nxt, r - 1)
                return carry

            def active_row(r, gr):

                def split_one(k, carry):
                    split_first(t, 30 + k, X[cur, gr, k], gr, k)
                    return carry

                lax.fori_loop(0, 10, split_one, 0)

                def one(jj, carry):
                    k = 5 + 2 * ((2 - jj) // 2) + ((jj + 1) // 2) * (3 * u + jj - 1)
                    new = on_square * product(30, jj * 10, NN) + on_old * old_tile(t, X[cur, gr, k], gr, k)
                    X[nxt, gr, k] = new

                    @pl.when(jnp.logical_and(jnp.logical_and(r == 0, jj == 0), t >= 1))
                    def _():
                        pl.semaphore_wait(credit.at[0], 1)
                        pl.semaphore_wait(credit.at[1], 1)

                        @pl.when(jnp.logical_and(inner == 1, t < steps - 1))
                        def _():
                            pl.semaphore_wait(credit.at[2], 1)

                    copy(x_tile(nxt, gr, k), x_tile(nxt, gr, k), send.at[nxt, 0], recv_x.at[nxt, gr], sib).start()

                    @pl.when(jj > 0)
                    def _():
                        copy(x_tile(nxt, gr, k), x_tile(nxt, gr, k), send.at[nxt, 1], recv_y.at[nxt, gr], ypart).start()
                    return carry

                lax.fori_loop(0, 3, one, 0)

            lax.fori_loop(0, 5, row, 0)

            @pl.when(t >= 1)
            def _():
                send1_drain(cur)

        line = lax.broadcasted_iota(jnp.int32, (8, 128), 0)
        squares = sum(jnp.sum(jnp.square(X[(cur, *there)])) for there, _ in own)

        @pl.when(t > 0)
        def _():
            stats[...] = jnp.where(line == t, squares, stats[...])

        @pl.when(t == 0)
        def _():
            start = scale * (jnp.where(row_id == col_id, mu, 0.0) - h_ref[...]) + jnp.where(row_id == col_id, shift, 0.0)
            stats[...] = jnp.where(line == 0, jnp.sum(start * start), stats[...])
            for index in (0, 1, 2, 3, 4, 6):
                wait_send(out_ref, g_send.at[index])

            @pl.when(over_y)
            def _():
                wait_send(out_ref, g_send.at[5])

            @pl.when(over_z)
            def _():
                wait_send(out_ref, g_send.at[7])

            @pl.when(inner == 1)
            def _():
                wait_send(D.at[0], g_send.at[8])

        @pl.when(t < steps - 1)
        def _():
            pl.semaphore_signal(credit.at[0], inc=1, device_id=sib, device_id_type=MESH)

            @pl.when(c == 1)
            def _():
                pl.semaphore_signal(credit.at[1], inc=1, device_id=ypart, device_id_type=MESH)

                @pl.when(t < steps - 2)
                def _():
                    @pl.when(inner == 1)
                    def _():
                        pl.semaphore_signal(credit.at[2], inc=1, device_id=dev(opp, sib_col), device_id_type=MESH)

                    @pl.when(inner == 0)
                    def _():
                        pl.semaphore_signal(credit.at[2], inc=1, device_id=dev(inner_z, col), device_id_type=MESH)
        return carry

    stats[...] = jnp.zeros_like(stats)
    lax.fori_loop(0, steps, step, 0)
    last = steps % 2

    @pl.when(jnp.logical_and(c == 1, member(4, plane)))
    def _():
        forward_x(last, 4)

    for r in range(5):
        active = member(r, plane)
        gr = slab_of(r)

        @pl.when(jnp.logical_and(c == 0, active))
        def _():
            wait_recv(X.at[last, gr, pl.ds(5, 5)], recv_x.at[last, gr])

        @pl.when(jnp.logical_and(jnp.logical_and(c == 1, u == 0), active))
        def _():
            wait_recv(X.at[last, gr, pl.ds(0, 5)], recv_x.at[last, gr])

        @pl.when(jnp.logical_and(jnp.logical_and(c == 1, u == 0), jnp.logical_not(active)))
        def _():
            wait_recv(X.at[last, gr, pl.ds(0, 3)], recv_x.at[last, gr])

    energy = jnp.float32(0.0)
    for there, here in own:
        final = X[(last, *there)]
        out_ref[here] = final
        energy += jnp.sum(final * h_ref[here])
    line = lax.broadcasted_iota(jnp.int32, (8, 128), 0)
    part1[me] = jnp.where(line == steps, energy, stats[...])
    share(part1)

    @pl.when(jnp.logical_and(c == 0, u == 0))
    def _():
        wait_send(twelve, send.at[last, 0])
        wait_send(nine, send.at[last, 1])

    @pl.when(c == 1)
    def _():
        wait_send(nine, send.at[last, 0])
        wait_send(six, send.at[last, 1])
        wait_send(six, send.at[last, 3])

    total = collect(part1)
    for t in range(steps):
        occ_ref[t] = total[t, 0]
    energy_ref[0] = 2.0 * total[steps, 0]


def solution(mesh):
    def local_run(ham_block, bounds, occ_count, branches):
        blk = ham_block.shape[0]
        steps = branches.shape[0]
        T = 2 * blk // 5
        vmem, smem = pl.BlockSpec(memory_space=pltpu.VMEM), pl.BlockSpec(memory_space=pltpu.SMEM)
        return pl.pallas_call(
            functools.partial(kernel, steps),
            out_shape=(jax.ShapeDtypeStruct((blk, blk), F32), jax.ShapeDtypeStruct((steps,), F32),
                       jax.ShapeDtypeStruct((1,), F32)),
            in_specs=[vmem, smem, smem, smem],
            out_specs=(vmem, smem, smem),
            scratch_shapes=[
                pltpu.VMEM((2, 5, 10, T, T), F32),
                pltpu.VMEM((2, 5, 3, T, T), F32),
                pltpu.VMEM((50, 3, T, T), BF16),
                pltpu.VMEM((8, 128), F32),
                pltpu.VMEM((16, 8, 128), F32),
                pltpu.VMEM((16, 8, 128), F32),
                pltpu.SemaphoreType.DMA((11,)),
                pltpu.SemaphoreType.DMA((11,)),
                pltpu.SemaphoreType.DMA((2, 4)),
                pltpu.SemaphoreType.DMA((2, 5)),
                pltpu.SemaphoreType.DMA((2, 5)),
                pltpu.SemaphoreType.DMA((2, 15)),
                pltpu.SemaphoreType.REGULAR((3,)),
                pltpu.SemaphoreType.DMA((15,)),
                pltpu.SemaphoreType.DMA((1,)),
            ],
            compiler_params=pltpu.CompilerParams(collective_id=0, has_side_effects=True, vmem_limit_bytes=67043328),
        )(ham_block, bounds, occ_count, branches)

    return jax.shard_map(local_run, mesh=mesh, in_specs=(P(("spin", "row"), "col"), P("spin"), P("spin"), P("spin")), out_specs=(P(("spin", "row"), "col"), P("spin"), P("spin")), check_vma=False)
```

```python
import functools

import jax
import jax.numpy as jnp
from jax import lax
from jax.experimental import pallas as pl
from jax.experimental.pallas import tpu as pltpu
from jax.sharding import PartitionSpec as P

F32 = jnp.float32
BF16 = jnp.bfloat16
MESH = pl.DeviceIdType.MESH
TERMS = ((0, 2), (2, 0), (1, 1), (0, 1), (1, 0), (0, 0))
NN = (((1,), (0,)), ((), ()))
NT = (((1,), (1,)), ((), ()))


def slab_of(label):
    return label // 2 + 2 * (1 - label % 2)


def kernel(steps, h_ref, bounds_ref, count_ref, flag_ref, out_ref, occ_ref, energy_ref,
           X, D, S, stats, part0, part1, g_send, g_recv, send, recv_x, recv_y, recv_d, credit, p_send, p_recv):
    blk = h_ref.shape[0]
    T = 2 * blk // 5
    order = 4 * blk
    sid, z, col = lax.axis_index("spin"), lax.axis_index("row"), lax.axis_index("col")
    y, c = col // 2, col % 2
    half = z // 2
    u = (y + half) % 2
    inner = (z + 1) // 2 % 2
    inner = jnp.int32(inner)
    sib_col, yp_col, sib_yp_col = 2 * y + 1 - c, 2 * (1 - y) + c, 2 * (1 - y) + 1 - c
    zp = z + 1 - 2 * (z % 2)
    opp = 3 - z
    outer = 3 * (z // 2)
    inner_z = 1 + half
    me = z * 4 + col

    def dev(zz, cc):
        return (sid, zz, cc)

    sib, ypart, zpart = dev(z, sib_col), dev(z, yp_col), dev(zp, col)

    def copy(src, dst, s_sem, r_sem, device):
        return pltpu.make_async_remote_copy(src_ref=src, dst_ref=dst, send_sem=s_sem, recv_sem=r_sem,
                                            device_id=device, device_id_type=MESH)

    def wait_recv(dst, r_sem):
        copy(dst, dst, g_send.at[0], r_sem, sib).wait_recv()

    def wait_send(src, s_sem):
        copy(src, src, s_sem, g_recv.at[0], sib).wait_send()

    Q = T // 2

    def spans(p):
        return ((3 * p, 0, p * Q, T), (3 * p + 1, 0, p * Q + T, T), (2, p * Q, (1 - p) * 2 * T, Q))

    def at(offset, size):
        return pl.ds(offset if isinstance(offset, int) else pl.multiple_of(offset, Q), size)

    def pieces(zz, cc):
        first = 5 * ((cc // 2 + zz // 2) % 2)
        out = []
        for row, r_in, r_at, r_size in spans(zz % 2):
            for column, c_in, c_at, c_size in spans(cc % 2):
                out.append(((row, first + column, at(r_in, r_size), at(c_in, c_size)),
                            (at(r_at, r_size), at(c_at, c_size))))
        return out

    own = pieces(z, col)

    def send_block(zz, cc, s_sem, r_sem, device, fresh=False):
        for there, here in pieces(zz, cc):
            dst = X.at[(0, *there)]
            copy(h_ref.at[here] if fresh else dst, dst, s_sem, r_sem, device).start()

    barrier = pltpu.get_barrier_semaphore()
    for dz in range(4):
        for dc in range(4):
            if dz or dc:
                pl.semaphore_signal(barrier, inc=1, device_id=dev((z + dz) % 4, (col + dc) % 4), device_id_type=MESH)
    pl.semaphore_wait(barrier, 15)

    def share(part):
        index = 0
        for dz in range(4):
            for dc in range(4):
                if dz or dc:
                    copy(part.at[me], part.at[me], p_send.at[index], p_recv.at[0],
                         dev((z + dz) % 4, (col + dc) % 4)).start()
                    index += 1

    def collect(part):
        wait_recv(part.at[pl.ds(0, 15)], p_recv.at[0])
        for index in range(15):
            wait_send(part.at[me], p_send.at[index])
        return jnp.sum(part[...], axis=0)

    send_block(z, col, g_send.at[1], g_recv.at[1], ypart, True)
    send_block(z, col, g_send.at[2], g_recv.at[2], zpart, True)
    send_block(z, col, g_send.at[0], g_recv.at[0], sib, True)
    for there, here in own:
        X[(0, *there)] = h_ref[here]
    row_id = lax.broadcasted_iota(jnp.int32, (blk, blk), 0) + z * blk
    col_id = lax.broadcasted_iota(jnp.int32, (blk, blk), 1) + col * blk
    part0[me] = jnp.full((8, 128), jnp.sum(jnp.where(row_id == col_id, h_ref[...], 0.0)), F32)
    share(part0)

    def wait_block(r_sem):
        wait_recv(out_ref, r_sem)

    def d_slab(index, zz):
        p = zz % 2
        return (3 * p, 3 * p + 1, 2, 3 * (1 - p), 3 * (1 - p) + 1)[index]

    def set_slab_of(jj, who):
        return (2, 3 * who, 3 * who + 1)[jj]

    def d_send(rows, when):
        @pl.when(jnp.logical_and(jnp.logical_and(c == 0, inner == 1), when))
        def _():
            for index in rows:
                row = d_slab(index, z)
                for jj in range(3):
                    copy(X.at[0, row, set_slab_of(jj, 1 - u)], D.at[0, row, jj], g_send.at[8],
                         recv_d.at[0, 3 * index + jj], dev(opp, sib_col)).start()

    def relay(rows, when):
        @pl.when(jnp.logical_and(c == 1, when))
        def _():
            for index in rows:
                row = d_slab(index, 3 - inner_z)
                for jj in range(3):
                    tile = D.at[0, row, jj]
                    wait_recv(tile, recv_d.at[0, 3 * index + jj])

                    @pl.when(inner == 1)
                    def _():
                        copy(tile, tile, g_send.at[8], recv_d.at[0, 3 * index + jj], dev(outer, col)).start()

    over_y = jnp.logical_or(inner == 0, c == 0)
    over_z = jnp.logical_and(inner == 0, c == 1)
    wait_block(g_recv.at[0])
    d_send((0, 1), u == 0)
    wait_block(g_recv.at[1])

    @pl.when(over_z)
    def _():
        send_block(z, yp_col, g_send.at[7], g_recv.at[5], zpart)

    send_block(z, yp_col, g_send.at[3], g_recv.at[3], sib)
    wait_block(g_recv.at[2])

    @pl.when(over_y)
    def _():
        send_block(zp, col, g_send.at[5], g_recv.at[5], ypart)

    send_block(zp, col, g_send.at[4], g_recv.at[4], sib)
    wait_block(g_recv.at[3])
    d_send((0, 1), u == 1)
    wait_block(g_recv.at[4])
    d_send((2, 3, 4), u == 0)
    early = jnp.logical_and(inner == 1, u == 1)
    relay((0, 1), early)
    wait_block(g_recv.at[5])
    send_block(zp, yp_col, g_send.at[6], g_recv.at[6], sib)
    wait_block(g_recv.at[6])
    d_send((2, 3, 4), u == 1)

    total = collect(part0)
    mu = total / order
    occupied = jnp.full((8, 128), count_ref[0], jnp.int32).astype(F32)
    scale = jnp.minimum(occupied / (bounds_ref[1] - mu), (order - occupied) / (mu - bounds_ref[0])) / order
    shift = occupied / order
    mu, scale, shift = mu[0:1, 0:1], scale[0:1, 0:1], shift[0:1, 0:1]

    iota_r = lax.broadcasted_iota(jnp.int32, (T, T), 0)
    iota_c = lax.broadcasted_iota(jnp.int32, (T, T), 1)

    def start_tile(tile, slab_r, slab_c):
        diag = iota_r + slab_r * T == iota_c + slab_c * T
        return scale * (jnp.where(diag, mu, 0.0) - tile) + jnp.where(diag, shift, 0.0)

    def set_slab(jj):
        return set_slab_of(jj, u)

    relay((0, 1), jnp.logical_not(early))
    relay((2, 3, 4), c == 1)

    first_on = -scale
    first_diag = scale * mu + shift

    def old_tile(t, tile, slab_r, slab_c):
        diag = iota_r + slab_r * T == iota_c + slab_c * T
        first = (t == 0).astype(jnp.int32).astype(F32)
        keep = 1.0 - first
        return (first * first_on + keep) * tile + jnp.where(diag, first * first_diag, 0.0)

    def split_first(t, index, tile, slab_r, slab_c):
        @pl.when(t == 0)
        def _():
            split(index, start_tile(tile, slab_r, slab_c))

        @pl.when(t > 0)
        def _():
            split(index, tile)

    def split(index, tile):
        first = tile.astype(BF16)
        rest = tile - first.astype(F32)
        second = rest.astype(BF16)
        S[index, 0] = first
        S[index, 1] = second
        S[index, 2] = (rest - second.astype(F32)).astype(BF16)

    def product(left, right, dims):
        acc = None
        for a, b in TERMS:
            for k in range(10):
                term = lax.dot_general(S[left + k, a], S[right + k, b], dims, preferred_element_type=F32)
                acc = term if acc is None else acc + term
        return acc

    def member(label, who):
        return jnp.logical_or(jnp.int32(label) == 0, label % 2 == 1 - who)

    def x_tile(par, r, k):
        return X.at[par, r, k]

    def d_tile(par, r, jj):
        return D.at[par, r, jj]

    def d_place(i, s, who):
        in_s = member(s, who)
        return jnp.where(in_s, slab_of(i), slab_of(s)), jnp.where(in_s, (s + 1) // 2, (i + 1) // 2)

    fifteen, twelve, ten, nine, six = (D.at[0], X.at[0, pl.ds(0, 4), pl.ds(0, 3)], X.at[0, 0],
                                       X.at[0, pl.ds(0, 3), pl.ds(0, 3)], X.at[0, pl.ds(0, 2), pl.ds(0, 3)])
    plane = z % 2

    def send0_drain(par):
        wait_send(fifteen, send.at[par, 0])
        wait_send(ten, send.at[par, 1])

        @pl.when(inner == 1)
        def _():
            wait_send(twelve, send.at[par, 2])

    def send1_drain(par):
        wait_send(fifteen, send.at[par, 0])
        wait_send(ten, send.at[par, 1])
        wait_send(ten, send.at[par, 3])

        @pl.when(inner == 1)
        def _():
            wait_send(twelve, send.at[par, 2])

    def forward_x(par, r):
        gr = slab_of(r)
        first = 5 + 3 * (1 - u)
        wait_recv(X.at[par, gr, pl.ds(first, 2)], recv_y.at[par, gr])
        for q in range(2):
            tile = x_tile(par, gr, first + q)
            copy(tile, tile, send.at[par, 3], recv_x.at[par, gr], sib).start()

    def forward_d(par, s, low, high):
        def one(i, carry):
            @pl.when(jnp.logical_or(member(s, u), member(i, u)))
            def _():
                row_slab, jj = d_place(i, s, u)
                tile = d_tile(par, row_slab, jj)
                wait_recv(tile, recv_d.at[par, 3 * row_slab + jj])

                @pl.when(inner == 1)
                def _():
                    copy(tile, tile, send.at[par, 2],
                         recv_d.at[par, 3 * row_slab + jj], dev(outer, col)).start()
            return carry
        lax.fori_loop(low, high, one, 0)

    def send_tile(t, nxt, s, i):
        gs, gi = slab_of(s), slab_of(i)
        s, i = jnp.int32(s), jnp.int32(i)
        who = 1 - u
        in_s = member(s, who)

        @pl.when(jnp.logical_and(jnp.logical_and(inner == 1, t < steps - 1), jnp.logical_or(in_s, member(i, who))))
        def _():
            row_slab, jj = d_place(i, s, who)
            src_r, src_c = jnp.where(in_s, gi, gs), jnp.where(in_s, gs, gi)
            copy(x_tile(nxt, src_r, src_c), d_tile(nxt, row_slab, jj), send.at[nxt, 2],
                 recv_d.at[nxt, 3 * row_slab + jj], dev(opp, sib_col)).start()

        copy(x_tile(nxt, gi, gs), x_tile(nxt, gi, gs), send.at[nxt, 0], recv_x.at[nxt, gi], sib).start()

        @pl.when(i < s)
        def _():
            copy(x_tile(nxt, gs, gi), x_tile(nxt, gs, gi), send.at[nxt, 1], recv_x.at[nxt, gs], sib).start()

    def step(t, carry):
        cur, nxt = t % 2, (t + 1) % 2
        flag = flag_ref[t].astype(F32)
        on_square, on_old = 2.0 * flag - 1.0, 2.0 - 2.0 * flag

        @pl.when(c == 0)
        def _():
            def stage(s, carry):
                gs = slab_of(s)

                @pl.when(t >= 1)
                def _():
                    wait_recv(X.at[cur, gs, pl.ds(5, 5)], recv_x.at[cur, gs])

                def split_one(k, carry):
                    split_first(t, s * 10 + k, X[cur, gs, k], gs, k)
                    return carry

                lax.fori_loop(0, 10, split_one, 0)

                def one(i, carry):
                    gi = slab_of(i)
                    new = on_square * product(i * 10, s * 10, NT) + on_old * old_tile(t, X[cur, gi, gs], gi, gs)
                    X[nxt, gi, gs] = new

                    @pl.when(i < s)
                    def _():
                        X[nxt, gs, gi] = X[nxt, gi, gs].T

                    return carry

                def needed(i, carry):
                    full = t < steps - 1
                    mine = jnp.logical_and(u == 0, jnp.logical_or(member(i, plane), member(s, plane)))

                    @pl.when(jnp.logical_or(full, mine))
                    def _():
                        one(i, carry)

                    @pl.when(s * (s + 1) // 2 + i == 2)
                    def _():
                        @pl.when(t >= 1)
                        def _():
                            pl.semaphore_wait(credit.at[0], 1)

                            @pl.when(jnp.logical_and(inner == 1, full))
                            def _():
                                pl.semaphore_wait(credit.at[2], 1)

                        @pl.when(jnp.logical_or(full, u == 0))
                        def _():
                            send_tile(t, nxt, 0, 0)
                            send_tile(t, nxt, 1, 0)

                    @pl.when(jnp.logical_and(s * (s + 1) // 2 + i >= 2, jnp.logical_or(full, mine)))
                    def _():
                        send_tile(t, nxt, s, i)
                    return carry

                return lax.fori_loop(0, s + 1, needed, carry)

            lax.fori_loop(0, 5, stage, 0)

            @pl.when(t >= 1)
            def _():
                send0_drain(cur)

        @pl.when(c == 1)
        def _():
            for jj in range(3):
                def split_o(k, carry):
                    split_first(t, jj * 10 + k, X[cur, k, 5 + set_slab(jj)], k, 5 + set_slab(jj))
                    return carry

                lax.fori_loop(0, 5, split_o, 0)

            @pl.when(t >= 1)
            def _():
                forward_x(cur, 4)
                forward_d(cur, 4, 2, 5)
                for a, b in ((1, 0), (2, 0), (2, 1)):
                    D[cur, set_slab(a), b] = D[cur, set_slab(b), a].T

            for jj in range(3):
                def split_p(k, carry):
                    split_first(t, jj * 10 + 5 + k, D[cur, k, jj], k, set_slab(jj))
                    return carry

                lax.fori_loop(0, 5, split_p, 0)

            def row(r, carry):
                gr = slab_of(r)

                @pl.when(t >= 1)
                def _():
                    wait_recv(X.at[cur, gr, pl.ds(0, 5)], recv_x.at[cur, gr])

                @pl.when(jnp.logical_or(t < steps - 1, member(r, plane)))
                def _():
                    active_row(r, gr)

                @pl.when(jnp.logical_and(t < steps - 1, r < 4))
                def _():
                    @pl.when(jnp.logical_and(inner == 1, jnp.logical_and(r == 0, t >= 1)))
                    def _():
                        pl.semaphore_wait(credit.at[2], 1)

                    forward_d(nxt, r, 0, r + 1)

                @pl.when(jnp.logical_and(r >= 1, jnp.logical_or(t < steps - 1, member(r - 1, plane))))
                def _():
                    forward_x(nxt, r - 1)
                return carry

            def active_row(r, gr):

                def split_one(k, carry):
                    split_first(t, 30 + k, X[cur, gr, k], gr, k)
                    return carry

                lax.fori_loop(0, 10, split_one, 0)

                def one(jj, carry):
                    k = 5 + 2 * ((2 - jj) // 2) + ((jj + 1) // 2) * (3 * u + jj - 1)
                    new = on_square * product(30, jj * 10, NN) + on_old * old_tile(t, X[cur, gr, k], gr, k)
                    X[nxt, gr, k] = new

                    @pl.when(jnp.logical_and(jnp.logical_and(r == 0, jj == 0), t >= 1))
                    def _():
                        pl.semaphore_wait(credit.at[0], 1)
                        pl.semaphore_wait(credit.at[1], 1)

                    copy(x_tile(nxt, gr, k), x_tile(nxt, gr, k), send.at[nxt, 0], recv_x.at[nxt, gr], sib).start()

                    @pl.when(jj > 0)
                    def _():
                        copy(x_tile(nxt, gr, k), x_tile(nxt, gr, k), send.at[nxt, 1], recv_y.at[nxt, gr], ypart).start()

                    @pl.when(jnp.logical_and(jnp.logical_and(r == 4, jj == 1), t < steps - 1))
                    def _():
                        forward_d(nxt, 4, 0, 2)
                    return carry

                lax.fori_loop(0, 3, one, 0)

            lax.fori_loop(0, 5, row, 0)

            @pl.when(t >= 1)
            def _():
                send1_drain(cur)

        line = lax.broadcasted_iota(jnp.int32, (8, 128), 0)
        squares = sum(jnp.sum(jnp.square(X[(cur, *there)])) for there, _ in own)

        @pl.when(t > 0)
        def _():
            stats[...] = jnp.where(line == t, squares, stats[...])

        @pl.when(t == 0)
        def _():
            start = scale * (jnp.where(row_id == col_id, mu, 0.0) - h_ref[...]) + jnp.where(row_id == col_id, shift, 0.0)
            stats[...] = jnp.where(line == 0, jnp.sum(start * start), stats[...])
            for index in (0, 1, 2, 3, 4, 6):
                wait_send(out_ref, g_send.at[index])

            @pl.when(over_y)
            def _():
                wait_send(out_ref, g_send.at[5])

            @pl.when(over_z)
            def _():
                wait_send(out_ref, g_send.at[7])

            @pl.when(inner == 1)
            def _():
                wait_send(D.at[0], g_send.at[8])

        @pl.when(t < steps - 1)
        def _():
            pl.semaphore_signal(credit.at[0], inc=1, device_id=sib, device_id_type=MESH)

            @pl.when(c == 1)
            def _():
                pl.semaphore_signal(credit.at[1], inc=1, device_id=ypart, device_id_type=MESH)

                @pl.when(t < steps - 2)
                def _():
                    @pl.when(inner == 1)
                    def _():
                        pl.semaphore_signal(credit.at[2], inc=1, device_id=dev(opp, sib_col), device_id_type=MESH)

                    @pl.when(inner == 0)
                    def _():
                        pl.semaphore_signal(credit.at[2], inc=1, device_id=dev(inner_z, col), device_id_type=MESH)
        return carry

    stats[...] = jnp.zeros_like(stats)
    lax.fori_loop(0, steps, step, 0)
    last = steps % 2

    @pl.when(jnp.logical_and(c == 1, member(4, plane)))
    def _():
        forward_x(last, 4)

    for r in range(5):
        active = member(r, plane)
        gr = slab_of(r)

        @pl.when(jnp.logical_and(c == 0, active))
        def _():
            wait_recv(X.at[last, gr, pl.ds(5, 5)], recv_x.at[last, gr])

        @pl.when(jnp.logical_and(jnp.logical_and(c == 1, u == 0), active))
        def _():
            wait_recv(X.at[last, gr, pl.ds(0, 5)], recv_x.at[last, gr])

        @pl.when(jnp.logical_and(jnp.logical_and(c == 1, u == 0), jnp.logical_not(active)))
        def _():
            wait_recv(X.at[last, gr, pl.ds(0, 3)], recv_x.at[last, gr])

    energy = jnp.float32(0.0)
    for there, here in own:
        final = X[(last, *there)]
        out_ref[here] = final
        energy += jnp.sum(final * h_ref[here])
    line = lax.broadcasted_iota(jnp.int32, (8, 128), 0)
    part1[me] = jnp.where(line == steps, energy, stats[...])
    share(part1)

    @pl.when(jnp.logical_and(c == 0, u == 0))
    def _():
        wait_send(twelve, send.at[last, 0])
        wait_send(nine, send.at[last, 1])

    @pl.when(c == 1)
    def _():
        wait_send(nine, send.at[last, 0])
        wait_send(six, send.at[last, 1])
        wait_send(six, send.at[last, 3])

    total = collect(part1)
    for t in range(steps):
        occ_ref[t] = total[t, 0]
    energy_ref[0] = 2.0 * total[steps, 0]


def solution(mesh):
    def local_run(ham_block, bounds, occ_count, branches):
        blk = ham_block.shape[0]
        steps = branches.shape[0]
        T = 2 * blk // 5
        vmem, smem = pl.BlockSpec(memory_space=pltpu.VMEM), pl.BlockSpec(memory_space=pltpu.SMEM)
        return pl.pallas_call(
            functools.partial(kernel, steps),
            out_shape=(jax.ShapeDtypeStruct((blk, blk), F32), jax.ShapeDtypeStruct((steps,), F32),
                       jax.ShapeDtypeStruct((1,), F32)),
            in_specs=[vmem, smem, smem, smem],
            out_specs=(vmem, smem, smem),
            scratch_shapes=[
                pltpu.VMEM((2, 5, 10, T, T), F32),
                pltpu.VMEM((2, 5, 3, T, T), F32),
                pltpu.VMEM((50, 3, T, T), BF16),
                pltpu.VMEM((8, 128), F32),
                pltpu.VMEM((16, 8, 128), F32),
                pltpu.VMEM((16, 8, 128), F32),
                pltpu.SemaphoreType.DMA((11,)),
                pltpu.SemaphoreType.DMA((11,)),
                pltpu.SemaphoreType.DMA((2, 4)),
                pltpu.SemaphoreType.DMA((2, 5)),
                pltpu.SemaphoreType.DMA((2, 5)),
                pltpu.SemaphoreType.DMA((2, 15)),
                pltpu.SemaphoreType.REGULAR((3,)),
                pltpu.SemaphoreType.DMA((15,)),
                pltpu.SemaphoreType.DMA((1,)),
            ],
            compiler_params=pltpu.CompilerParams(collective_id=0, has_side_effects=True, vmem_limit_bytes=67043328),
        )(ham_block, bounds, occ_count, branches)

    return jax.shard_map(local_run, mesh=mesh, in_specs=(P(("spin", "row"), "col"), P("spin"), P("spin"), P("spin")), out_specs=(P(("spin", "row"), "col"), P("spin"), P("spin")), check_vma=False)
```

```python
import functools

import jax
import jax.numpy as jnp
from jax import lax
from jax.experimental import pallas as pl
from jax.experimental.pallas import tpu as pltpu
from jax.sharding import PartitionSpec as P

F32 = jnp.float32
BF16 = jnp.bfloat16
MESH = pl.DeviceIdType.MESH
TERMS = ((0, 2), (2, 0), (1, 1), (0, 1), (1, 0), (0, 0))
NN = (((1,), (0,)), ((), ()))
NT = (((1,), (1,)), ((), ()))


def slab_of(label):
    return label // 2 + 2 * (1 - label % 2)


def kernel(steps, h_ref, bounds_ref, count_ref, flag_ref, out_ref, occ_ref, energy_ref,
           X, D, S, stats, part0, part1, g_send, g_recv, send, recv_x, recv_y, recv_d, credit, p_send, p_recv):
    blk = h_ref.shape[0]
    T = 2 * blk // 5
    order = 4 * blk
    sid, z, col = lax.axis_index("spin"), lax.axis_index("row"), lax.axis_index("col")
    y, c = col // 2, col % 2
    half = z // 2
    u = (y + half) % 2
    inner = (z + 1) // 2 % 2
    inner = jnp.int32(inner)
    sib_col, yp_col, sib_yp_col = 2 * y + 1 - c, 2 * (1 - y) + c, 2 * (1 - y) + 1 - c
    zp = z + 1 - 2 * (z % 2)
    opp = 3 - z
    outer = 3 * (z // 2)
    inner_z = 1 + half
    me = z * 4 + col

    def dev(zz, cc):
        return (sid, zz, cc)

    sib, ypart, zpart = dev(z, sib_col), dev(z, yp_col), dev(zp, col)

    def copy(src, dst, s_sem, r_sem, device):
        return pltpu.make_async_remote_copy(src_ref=src, dst_ref=dst, send_sem=s_sem, recv_sem=r_sem,
                                            device_id=device, device_id_type=MESH)

    def wait_recv(dst, r_sem):
        copy(dst, dst, g_send.at[0], r_sem, sib).wait_recv()

    def wait_send(src, s_sem):
        copy(src, src, s_sem, g_recv.at[0], sib).wait_send()

    Q = T // 2

    def spans(p):
        return ((3 * p, 0, p * Q, T), (3 * p + 1, 0, p * Q + T, T), (2, p * Q, (1 - p) * 2 * T, Q))

    def at(offset, size):
        return pl.ds(offset if isinstance(offset, int) else pl.multiple_of(offset, Q), size)

    def pieces(zz, cc):
        first = 5 * ((cc // 2 + zz // 2) % 2)
        out = []
        for row, r_in, r_at, r_size in spans(zz % 2):
            for column, c_in, c_at, c_size in spans(cc % 2):
                out.append(((row, first + column, at(r_in, r_size), at(c_in, c_size)),
                            (at(r_at, r_size), at(c_at, c_size))))
        return out

    own = pieces(z, col)

    def send_block(zz, cc, s_sem, r_sem, device, fresh=False):
        for there, here in pieces(zz, cc):
            dst = X.at[(0, *there)]
            copy(h_ref.at[here] if fresh else dst, dst, s_sem, r_sem, device).start()

    barrier = pltpu.get_barrier_semaphore()
    for dz in range(4):
        for dc in range(4):
            if dz or dc:
                pl.semaphore_signal(barrier, inc=1, device_id=dev((z + dz) % 4, (col + dc) % 4), device_id_type=MESH)
    pl.semaphore_wait(barrier, 15)

    def share(part):
        index = 0
        for dz in range(4):
            for dc in range(4):
                if dz or dc:
                    copy(part.at[me], part.at[me], p_send.at[index], p_recv.at[0],
                         dev((z + dz) % 4, (col + dc) % 4)).start()
                    index += 1

    def collect(part):
        wait_recv(part.at[pl.ds(0, 15)], p_recv.at[0])
        for index in range(15):
            wait_send(part.at[me], p_send.at[index])
        return jnp.sum(part[...], axis=0)

    send_block(z, col, g_send.at[1], g_recv.at[1], ypart, True)
    send_block(z, col, g_send.at[2], g_recv.at[2], zpart, True)
    send_block(z, col, g_send.at[0], g_recv.at[0], sib, True)
    for there, here in own:
        X[(0, *there)] = h_ref[here]
    row_id = lax.broadcasted_iota(jnp.int32, (blk, blk), 0) + z * blk
    col_id = lax.broadcasted_iota(jnp.int32, (blk, blk), 1) + col * blk
    part0[me] = jnp.full((8, 128), jnp.sum(jnp.where(row_id == col_id, h_ref[...], 0.0)), F32)
    share(part0)

    def wait_block(r_sem):
        wait_recv(out_ref, r_sem)

    def d_slab(index, zz):
        p = zz % 2
        return (3 * p, 3 * p + 1, 2, 3 * (1 - p), 3 * (1 - p) + 1)[index]

    def set_slab_of(jj, who):
        return (2, 3 * who, 3 * who + 1)[jj]

    def d_send(rows, when):
        @pl.when(jnp.logical_and(jnp.logical_and(c == 0, inner == 1), when))
        def _():
            for index in rows:
                row = d_slab(index, z)
                for jj in range(3):
                    copy(X.at[0, row, set_slab_of(jj, 1 - u)], D.at[0, row, jj], g_send.at[8],
                         recv_d.at[0, 3 * index + jj], dev(opp, sib_col)).start()

    def relay(rows, when):
        @pl.when(jnp.logical_and(c == 1, when))
        def _():
            for index in rows:
                row = d_slab(index, 3 - inner_z)
                for jj in range(3):
                    tile = D.at[0, row, jj]
                    wait_recv(tile, recv_d.at[0, 3 * index + jj])

                    @pl.when(inner == 1)
                    def _():
                        copy(tile, tile, g_send.at[8], recv_d.at[0, 3 * index + jj], dev(outer, col)).start()

    over_y = jnp.logical_or(inner == 0, c == 0)
    over_z = jnp.logical_and(inner == 0, c == 1)
    wait_block(g_recv.at[0])
    d_send((0, 1), u == 0)
    wait_block(g_recv.at[1])

    @pl.when(over_z)
    def _():
        send_block(z, yp_col, g_send.at[7], g_recv.at[5], zpart)

    send_block(z, yp_col, g_send.at[3], g_recv.at[3], sib)
    wait_block(g_recv.at[2])

    @pl.when(over_y)
    def _():
        send_block(zp, col, g_send.at[5], g_recv.at[5], ypart)

    send_block(zp, col, g_send.at[4], g_recv.at[4], sib)
    wait_block(g_recv.at[3])
    d_send((0, 1), u == 1)
    wait_block(g_recv.at[4])
    d_send((2, 3, 4), u == 0)
    early = jnp.logical_and(inner == 1, u == 1)
    relay((0, 1), early)
    wait_block(g_recv.at[5])
    send_block(zp, yp_col, g_send.at[6], g_recv.at[6], sib)
    wait_block(g_recv.at[6])
    d_send((2, 3, 4), u == 1)

    total = collect(part0)
    mu = total / order
    occupied = jnp.full((8, 128), count_ref[0], jnp.int32).astype(F32)
    scale = jnp.minimum(occupied / (bounds_ref[1] - mu), (order - occupied) / (mu - bounds_ref[0])) / order
    shift = occupied / order
    mu, scale, shift = mu[0:1, 0:1], scale[0:1, 0:1], shift[0:1, 0:1]

    iota_r = lax.broadcasted_iota(jnp.int32, (T, T), 0)
    iota_c = lax.broadcasted_iota(jnp.int32, (T, T), 1)

    def start_tile(tile, slab_r, slab_c):
        diag = iota_r + slab_r * T == iota_c + slab_c * T
        return scale * (jnp.where(diag, mu, 0.0) - tile) + jnp.where(diag, shift, 0.0)

    def set_slab(jj):
        return set_slab_of(jj, u)

    relay((0, 1), jnp.logical_not(early))
    relay((2, 3, 4), c == 1)

    first_on = -scale
    first_diag = scale * mu + shift

    def old_tile(t, tile, slab_r, slab_c):
        diag = iota_r + slab_r * T == iota_c + slab_c * T
        first = (t == 0).astype(jnp.int32).astype(F32)
        keep = 1.0 - first
        return (first * first_on + keep) * tile + jnp.where(diag, first * first_diag, 0.0)

    def split_first(t, index, tile, slab_r, slab_c):
        @pl.when(t == 0)
        def _():
            split(index, start_tile(tile, slab_r, slab_c))

        @pl.when(t > 0)
        def _():
            split(index, tile)

    def split(index, tile):
        first = tile.astype(BF16)
        rest = tile - first.astype(F32)
        second = rest.astype(BF16)
        S[index, 0] = first
        S[index, 1] = second
        S[index, 2] = (rest - second.astype(F32)).astype(BF16)

    def product(left, right, dims):
        acc = None
        for a, b in TERMS:
            for k in range(10):
                term = lax.dot_general(S[left + k, a], S[right + k, b], dims, preferred_element_type=F32)
                acc = term if acc is None else acc + term
        return acc

    def member(label, who):
        return jnp.logical_or(jnp.int32(label) == 0, label % 2 == 1 - who)

    def x_tile(par, r, k):
        return X.at[par, r, k]

    def d_tile(par, r, jj):
        return D.at[par, r, jj]

    def d_place(i, s, who):
        in_s = member(s, who)
        return jnp.where(in_s, slab_of(i), slab_of(s)), jnp.where(in_s, (s + 1) // 2, (i + 1) // 2)

    fifteen, twelve, ten, nine, six = (D.at[0], X.at[0, pl.ds(0, 4), pl.ds(0, 3)], X.at[0, 0],
                                       X.at[0, pl.ds(0, 3), pl.ds(0, 3)], X.at[0, pl.ds(0, 2), pl.ds(0, 3)])
    plane = z % 2

    def send0_drain(par):
        wait_send(fifteen, send.at[par, 0])
        wait_send(ten, send.at[par, 1])

        @pl.when(inner == 1)
        def _():
            wait_send(twelve, send.at[par, 2])

    def send1_drain(par):
        wait_send(fifteen, send.at[par, 0])
        wait_send(ten, send.at[par, 1])
        wait_send(ten, send.at[par, 3])

        @pl.when(inner == 1)
        def _():
            wait_send(twelve, send.at[par, 2])

    def forward_x(par, r):
        gr = slab_of(r)
        first = 5 + 3 * (1 - u)
        wait_recv(X.at[par, gr, pl.ds(first, 2)], recv_y.at[par, gr])
        for q in range(2):
            tile = x_tile(par, gr, first + q)
            copy(tile, tile, send.at[par, 3], recv_x.at[par, gr], sib).start()

    def forward_d(par, s, low, high):
        def one(i, carry):
            @pl.when(jnp.logical_or(member(s, u), member(i, u)))
            def _():
                row_slab, jj = d_place(i, s, u)
                tile = d_tile(par, row_slab, jj)
                wait_recv(tile, recv_d.at[par, 3 * row_slab + jj])

                @pl.when(inner == 1)
                def _():
                    copy(tile, tile, send.at[par, 2],
                         recv_d.at[par, 3 * row_slab + jj], dev(outer, col)).start()
            return carry
        lax.fori_loop(low, high, one, 0)

    def send_tile(t, nxt, s, i):
        gs, gi = slab_of(s), slab_of(i)
        s, i = jnp.int32(s), jnp.int32(i)
        who = 1 - u
        in_s = member(s, who)

        @pl.when(jnp.logical_and(jnp.logical_and(inner == 1, t < steps - 1), jnp.logical_or(in_s, member(i, who))))
        def _():
            row_slab, jj = d_place(i, s, who)
            src_r, src_c = jnp.where(in_s, gi, gs), jnp.where(in_s, gs, gi)
            copy(x_tile(nxt, src_r, src_c), d_tile(nxt, row_slab, jj), send.at[nxt, 2],
                 recv_d.at[nxt, 3 * row_slab + jj], dev(opp, sib_col)).start()

        copy(x_tile(nxt, gi, gs), x_tile(nxt, gi, gs), send.at[nxt, 0], recv_x.at[nxt, gi], sib).start()

        @pl.when(i < s)
        def _():
            copy(x_tile(nxt, gs, gi), x_tile(nxt, gs, gi), send.at[nxt, 1], recv_x.at[nxt, gs], sib).start()

    def step(t, carry):
        cur, nxt = t % 2, (t + 1) % 2
        flag = flag_ref[t].astype(F32)
        on_square, on_old = 2.0 * flag - 1.0, 2.0 - 2.0 * flag

        @pl.when(c == 0)
        def _():
            def stage(s, carry):
                gs = slab_of(s)

                @pl.when(t >= 1)
                def _():
                    wait_recv(X.at[cur, gs, pl.ds(5, 5)], recv_x.at[cur, gs])

                def split_one(k, carry):
                    split_first(t, s * 10 + k, X[cur, gs, k], gs, k)
                    return carry

                lax.fori_loop(0, 10, split_one, 0)

                def one(i, carry):
                    gi = slab_of(i)
                    new = on_square * product(i * 10, s * 10, NT) + on_old * old_tile(t, X[cur, gi, gs], gi, gs)
                    X[nxt, gi, gs] = new

                    @pl.when(i < s)
                    def _():
                        X[nxt, gs, gi] = X[nxt, gi, gs].T

                    return carry

                def needed(i, carry):
                    full = t < steps - 1
                    mine = jnp.logical_and(u == 0, jnp.logical_or(member(i, plane), member(s, plane)))

                    @pl.when(jnp.logical_or(full, mine))
                    def _():
                        one(i, carry)

                    @pl.when(s * (s + 1) // 2 + i == 2)
                    def _():
                        @pl.when(t >= 1)
                        def _():
                            pl.semaphore_wait(credit.at[0], 1)

                            @pl.when(jnp.logical_and(inner == 1, full))
                            def _():
                                pl.semaphore_wait(credit.at[2], 1)

                        @pl.when(jnp.logical_or(full, u == 0))
                        def _():
                            send_tile(t, nxt, 0, 0)
                            send_tile(t, nxt, 1, 0)

                    @pl.when(jnp.logical_and(s * (s + 1) // 2 + i >= 2, jnp.logical_or(full, mine)))
                    def _():
                        send_tile(t, nxt, s, i)
                    return carry

                return lax.fori_loop(0, s + 1, needed, carry)

            lax.fori_loop(0, 5, stage, 0)

            @pl.when(t >= 1)
            def _():
                send0_drain(cur)

        @pl.when(c == 1)
        def _():
            for jj in range(3):
                def split_o(k, carry):
                    split_first(t, jj * 10 + k, X[cur, k, 5 + set_slab(jj)], k, 5 + set_slab(jj))
                    return carry

                lax.fori_loop(0, 5, split_o, 0)

            @pl.when(t >= 1)
            def _():
                forward_x(cur, 4)
                forward_d(cur, 4, 3, 5)
                for a, b in ((1, 0), (2, 0), (2, 1)):
                    D[cur, set_slab(a), b] = D[cur, set_slab(b), a].T

            for jj in range(3):
                def split_p(k, carry):
                    split_first(t, jj * 10 + 5 + k, D[cur, k, jj], k, set_slab(jj))
                    return carry

                lax.fori_loop(0, 5, split_p, 0)

            def row(r, carry):
                gr = slab_of(r)

                @pl.when(t >= 1)
                def _():
                    wait_recv(X.at[cur, gr, pl.ds(0, 5)], recv_x.at[cur, gr])

                @pl.when(jnp.logical_or(t < steps - 1, member(r, plane)))
                def _():
                    active_row(r, gr)

                @pl.when(jnp.logical_and(r >= 1, jnp.logical_or(t < steps - 1, member(r - 1, plane))))
                def _():
                    forward_x(nxt, r - 1)
                return carry

            def active_row(r, gr):

                def split_one(k, carry):
                    split_first(t, 30 + k, X[cur, gr, k], gr, k)
                    return carry

                lax.fori_loop(0, 10, split_one, 0)

                def one(jj, carry):
                    k = 5 + 2 * ((2 - jj) // 2) + ((jj + 1) // 2) * (3 * u + jj - 1)
                    new = on_square * product(30, jj * 10, NN) + on_old * old_tile(t, X[cur, gr, k], gr, k)
                    X[nxt, gr, k] = new

                    @pl.when(jnp.logical_and(jnp.logical_and(r == 0, jj == 0), t >= 1))
                    def _():
                        pl.semaphore_wait(credit.at[0], 1)
                        pl.semaphore_wait(credit.at[1], 1)

                    copy(x_tile(nxt, gr, k), x_tile(nxt, gr, k), send.at[nxt, 0], recv_x.at[nxt, gr], sib).start()

                    @pl.when(jj > 0)
                    def _():
                        copy(x_tile(nxt, gr, k), x_tile(nxt, gr, k), send.at[nxt, 1], recv_y.at[nxt, gr], ypart).start()

                    @pl.when(jnp.logical_and(jj == 1, t < steps - 1))
                    def _():
                        @pl.when(jnp.logical_and(inner == 1, jnp.logical_and(r == 0, t >= 1)))
                        def _():
                            pl.semaphore_wait(credit.at[2], 1)

                        forward_d(nxt, r, 0, r + 1 - 2 * (r // 4))
                    return carry

                lax.fori_loop(0, 3, one, 0)

            lax.fori_loop(0, 5, row, 0)

            @pl.when(t >= 1)
            def _():
                send1_drain(cur)

        line = lax.broadcasted_iota(jnp.int32, (8, 128), 0)
        squares = sum(jnp.sum(jnp.square(X[(cur, *there)])) for there, _ in own)

        @pl.when(t > 0)
        def _():
            stats[...] = jnp.where(line == t, squares, stats[...])

        @pl.when(t == 0)
        def _():
            start = scale * (jnp.where(row_id == col_id, mu, 0.0) - h_ref[...]) + jnp.where(row_id == col_id, shift, 0.0)
            stats[...] = jnp.where(line == 0, jnp.sum(start * start), stats[...])
            for index in (0, 1, 2, 3, 4, 6):
                wait_send(out_ref, g_send.at[index])

            @pl.when(over_y)
            def _():
                wait_send(out_ref, g_send.at[5])

            @pl.when(over_z)
            def _():
                wait_send(out_ref, g_send.at[7])

            @pl.when(inner == 1)
            def _():
                wait_send(D.at[0], g_send.at[8])

        @pl.when(t < steps - 1)
        def _():
            pl.semaphore_signal(credit.at[0], inc=1, device_id=sib, device_id_type=MESH)

            @pl.when(c == 1)
            def _():
                pl.semaphore_signal(credit.at[1], inc=1, device_id=ypart, device_id_type=MESH)

                @pl.when(t < steps - 2)
                def _():
                    @pl.when(inner == 1)
                    def _():
                        pl.semaphore_signal(credit.at[2], inc=1, device_id=dev(opp, sib_col), device_id_type=MESH)

                    @pl.when(inner == 0)
                    def _():
                        pl.semaphore_signal(credit.at[2], inc=1, device_id=dev(inner_z, col), device_id_type=MESH)
        return carry

    stats[...] = jnp.zeros_like(stats)
    lax.fori_loop(0, steps, step, 0)
    last = steps % 2

    @pl.when(jnp.logical_and(c == 1, member(4, plane)))
    def _():
        forward_x(last, 4)

    for r in range(5):
        active = member(r, plane)
        gr = slab_of(r)

        @pl.when(jnp.logical_and(c == 0, active))
        def _():
            wait_recv(X.at[last, gr, pl.ds(5, 5)], recv_x.at[last, gr])

        @pl.when(jnp.logical_and(jnp.logical_and(c == 1, u == 0), active))
        def _():
            wait_recv(X.at[last, gr, pl.ds(0, 5)], recv_x.at[last, gr])

        @pl.when(jnp.logical_and(jnp.logical_and(c == 1, u == 0), jnp.logical_not(active)))
        def _():
            wait_recv(X.at[last, gr, pl.ds(0, 3)], recv_x.at[last, gr])

    energy = jnp.float32(0.0)
    for there, here in own:
        final = X[(last, *there)]
        out_ref[here] = final
        energy += jnp.sum(final * h_ref[here])
    line = lax.broadcasted_iota(jnp.int32, (8, 128), 0)
    part1[me] = jnp.where(line == steps, energy, stats[...])
    share(part1)

    @pl.when(jnp.logical_and(c == 0, u == 0))
    def _():
        wait_send(twelve, send.at[last, 0])
        wait_send(nine, send.at[last, 1])

    @pl.when(c == 1)
    def _():
        wait_send(nine, send.at[last, 0])
        wait_send(six, send.at[last, 1])
        wait_send(six, send.at[last, 3])

    total = collect(part1)
    for t in range(steps):
        occ_ref[t] = total[t, 0]
    energy_ref[0] = 2.0 * total[steps, 0]


def solution(mesh):
    def local_run(ham_block, bounds, occ_count, branches):
        blk = ham_block.shape[0]
        steps = branches.shape[0]
        T = 2 * blk // 5
        vmem, smem = pl.BlockSpec(memory_space=pltpu.VMEM), pl.BlockSpec(memory_space=pltpu.SMEM)
        return pl.pallas_call(
            functools.partial(kernel, steps),
            out_shape=(jax.ShapeDtypeStruct((blk, blk), F32), jax.ShapeDtypeStruct((steps,), F32),
                       jax.ShapeDtypeStruct((1,), F32)),
            in_specs=[vmem, smem, smem, smem],
            out_specs=(vmem, smem, smem),
            scratch_shapes=[
                pltpu.VMEM((2, 5, 10, T, T), F32),
                pltpu.VMEM((2, 5, 3, T, T), F32),
                pltpu.VMEM((50, 3, T, T), BF16),
                pltpu.VMEM((8, 128), F32),
                pltpu.VMEM((16, 8, 128), F32),
                pltpu.VMEM((16, 8, 128), F32),
                pltpu.SemaphoreType.DMA((11,)),
                pltpu.SemaphoreType.DMA((11,)),
                pltpu.SemaphoreType.DMA((2, 4)),
                pltpu.SemaphoreType.DMA((2, 5)),
                pltpu.SemaphoreType.DMA((2, 5)),
                pltpu.SemaphoreType.DMA((2, 15)),
                pltpu.SemaphoreType.REGULAR((3,)),
                pltpu.SemaphoreType.DMA((15,)),
                pltpu.SemaphoreType.DMA((1,)),
            ],
            compiler_params=pltpu.CompilerParams(collective_id=0, has_side_effects=True, vmem_limit_bytes=67043328),
        )(ham_block, bounds, occ_count, branches)

    return jax.shard_map(local_run, mesh=mesh, in_specs=(P(("spin", "row"), "col"), P("spin"), P("spin"), P("spin")), out_specs=(P(("spin", "row"), "col"), P("spin"), P("spin")), check_vma=False)
```
